256 devices in a mesh: pipe: 4 (over x), seq: 64 (over z, y, core).
Axes of the slice: x: 4, y: 4, z: 8, core: 2. Of those that a mesh axis runs over, the one named last changes fastest.
Arguments:
- previous: bfloat16 [4, 8192, 8192], P('pipe', 'seq'), may hold values from -6 to 6
- saved_head_inputs: bfloat16 [4, 8192, 8192], P('pipe', 'seq'), may hold values from -0.29882812 to 0.29882812
- input_b: bfloat16 [4, 8192, 1024], P('pipe', 'seq'), may hold values from -0.5 to 0.5
- input_c: bfloat16 [4, 8192, 1024], P('pipe', 'seq'), may hold values from -0.5 to 0.5
- steps: float32 [4, 8192, 128], P('pipe', 'seq'), may hold values from 0.1 to 13107.2, as said below
- decay_rate: float32 [4, 128], P('pipe'), may hold values from 3.0517578e-05 to 0.05
- skip_gain: float32 [4, 128], P('pipe'), may hold values from 0.5 to 1.5
- segment_ids: int32 [4, 8192], P('pipe', 'seq'), may hold values from 0 to 7, never falling along the last dimension, each value on 1 to 4096 neighbouring positions
- advantage_mask: int32 [8192], P('seq'), may hold values 0 or 1
Outputs:
- grad_x: bfloat16 [4, 8192, 8192], P('pipe', 'seq')
- grad_b: bfloat16 [4, 8192, 1024], P('pipe', 'seq')
- grad_c: bfloat16 [4, 8192, 1024], P('pipe', 'seq')
- bypass_gain_adjoint: float32 [4, 128], P('pipe')
The draws below stay inside these ranges and needn't reach their ends.
Inputs may be any that keep to these rules, and one draw needn't show every extreme that they name: `steps`: Positive; in a few positions of each section the step is 1.6 * 8192 for every head.
All inputs are finite; a program needn't handle non-finite values. No bound on the sum of `advantage_mask` on one device may be relied on, other than what follows from the above.
Results may differ from the reference program's by a relative error of at most 0.0095.
Values may be sent and summed in bfloat16 or wider, within the bound.
A program may use at most 128 MiB of HBM per device.

```python
import math
import jax
import jax.numpy as jnp
import numpy as np
from jax import lax

HEADS = 128
HEAD_DIM = 64
STATE = 128
GROUPS = 8
BLOCK = 256
TOK_DEV = 128
MERGED_POSITIONS = 8192
N_PIPE = 4
N_SEQ = 64


def draw_steps(key, part):
    first, second, tertiary_multiplier = jax.random.split(key, 3)
    starting_position = jax.random.uniform(first, (N_PIPE, MERGED_POSITIONS, HEADS), jnp.float32, 0.5, 2.0)
    factor = jax.random.uniform(second, (N_PIPE, MERGED_POSITIONS // TOK_DEV, 1, 1), jnp.float32, 1.0, 2.5)
    starting_position = (starting_position.reshape(N_PIPE, MERGED_POSITIONS // TOK_DEV, TOK_DEV, HEADS) * factor).reshape(N_PIPE, MERGED_POSITIONS, HEADS)
    relay_interval = jax.random.randint(tertiary_multiplier, (N_PIPE, MERGED_POSITIONS, 1), 0, max(MERGED_POSITIONS // 4, 1)) == 0
    return jnp.where(relay_interval, jnp.float32(1.6 * MERGED_POSITIONS), starting_position)


def with_ends(entries, stream_key, low, top_value):
    longest = entries.shape.index(max(entries.shape))
    spots = []
    for shift in (0, 1):
        where = [jax.random.randint(jax.random.fold_in(stream_key, axis), (), 0, length) for axis, length in enumerate(entries.shape)]
        where[longest] = (where[longest] + shift) % entries.shape[longest]
        spots.append(tuple(where))
    return entries.at[spots[0]].set(low).at[spots[1]].set(top_value)


def levels(key, shape, cuts, low, high):
    level = 1.0
    for position, shards_of in cuts:
        heights = jax.random.uniform(jax.random.fold_in(jax.random.fold_in(key, 6), position), (shards_of,), jnp.float32, low / len(cuts), high / len(cuts))
        level = level * jnp.repeat(jnp.exp(heights), shape[position] // shards_of).reshape((-1,) + (1,) * (len(shape) - 1 - position))
    return level


def length_profile(count, total, bound, slope):
    portions = [(1 << 20) // math.isqrt(standing ** slope) + 1 for standing in range(2, count + 1)]
    spare, holding = total - bound - (count - 1), [1] * (count - 1)
    while spare > 0:
        free = [i for i in range(count - 1) if holding[i] < bound]
        pool, left = sum([portions[i] for i in free]), spare
        for i in free:
            more = min(bound - holding[i], max(1, left * portions[i] // pool), spare)
            holding[i] = holding[i] + more
            spare = spare - more
    return np.array([bound] + holding)


def ragged(own_key, number_of, total, most, lean):
    if number_of == 2:
        one = jax.random.randint(own_key, (), max(1, total - most), min(most, total - 1) + 1)
        return jnp.stack([one, total - one])
    lengths = jnp.asarray(length_profile(number_of, total, most, lean), jnp.int32)
    pairs = (number_of - 1) // 2
    donor, sink = lengths[1:1 + 2 * pairs:2], lengths[2:2 + 2 * pairs:2]
    margin = jnp.minimum(donor - 1, most - sink)
    shifted = jax.random.randint(jax.random.fold_in(own_key, 1), (pairs,), 0, 1 << 20) % (margin + 1)
    lengths = lengths.at[1:1 + 2 * pairs:2].set(donor - shifted).at[2:2 + 2 * pairs:2].set(sink + shifted)
    return lengths[jax.random.permutation(jax.random.fold_in(own_key, 2), number_of)]


def scatter_about(key, dims, deviation, most, cuts=(), dtype=jnp.bfloat16):
    loudness = levels(key, dims, cuts, -0.22, 0.18) if cuts else 1.0
    result = jax.random.normal(key, dims, jnp.float32) * deviation * loudness
    return jnp.minimum(jnp.maximum(result, -most), most).astype(dtype)


def setup_inputs(seed: int = 0) -> dict:
    arg_keys = jax.random.split(jax.random.key(seed), 10)
    return {
        "previous": scatter_about(arg_keys[0], (N_PIPE, MERGED_POSITIONS, HEADS * HEAD_DIM), 1.0, 6.0, ((0, 4), (1, 64))),
        "saved_head_inputs": scatter_about(arg_keys[1], (N_PIPE, MERGED_POSITIONS, HEADS * HEAD_DIM), 0.05, 0.29882812, ((0, 4), (1, 64))),
        "input_b": scatter_about(arg_keys[2], (N_PIPE, MERGED_POSITIONS, GROUPS * STATE), STATE ** -0.5, 0.5, ((0, 4), (1, 64))),
        "input_c": scatter_about(arg_keys[3], (N_PIPE, MERGED_POSITIONS, GROUPS * STATE), STATE ** -0.5, 0.5, ((0, 4), (1, 64))),
        "steps": draw_steps(jax.random.fold_in(arg_keys[9], 71), 0),
        "decay_rate": jnp.clip(jnp.exp(math.log(0.05) - 7.4014754 * jax.random.uniform(arg_keys[5], (N_PIPE, HEADS), jnp.float32) ** levels(arg_keys[5], (N_PIPE, HEADS), ((0, 4),), -0.2, 0.2)), 3.0517578125e-05, 0.05),
        "skip_gain": jnp.clip(1.0 + 0.1 * jax.random.normal(arg_keys[6], (N_PIPE, HEADS), jnp.float32), 0.5, 1.5),
        "segment_ids": jax.vmap(lambda own: jnp.searchsorted(jnp.cumsum(ragged(own, max(2, N_SEQ // 8), MERGED_POSITIONS, MERGED_POSITIONS // 2, 1)), jnp.arange(MERGED_POSITIONS), side="right"))(jax.random.split(arg_keys[7], N_PIPE)).reshape((N_PIPE, MERGED_POSITIONS)).astype(jnp.int32),
        "advantage_mask": with_ends((jax.random.randint(arg_keys[8], (MERGED_POSITIONS,), 0, 4) < 3).astype(jnp.int32), jax.random.fold_in(arg_keys[8], 1), 0, 1),
    }


def mix(form, left, right):
    return jnp.einsum(form, left.astype(jnp.float32), right.astype(jnp.float32))


def prepare(seg, prev, steps_here, rate):
    length = seg.shape[0]
    cum = jnp.cumsum(-steps_here * rate[None, :], axis=0)
    row = lax.broadcasted_iota(jnp.int32, (length, length), 0)
    col = lax.broadcasted_iota(jnp.int32, (length, length), 1)
    link = (seg[:, None] == seg[None, :]) & (row >= col)
    spread = cum[:, None, :] - cum[None, :, :]
    kernel = jnp.exp(jnp.where(link[:, :, None], spread, -1e30))
    enter = jnp.exp(cum) * (seg == prev)[:, None].astype(jnp.float32)
    leave = jnp.exp(cum[-1][None, :] - cum) * (seg == seg[-1])[:, None].astype(jnp.float32)
    through = jnp.exp(cum[-1]) * (seg[-1] == prev).astype(jnp.float32)
    return kernel, enter, leave, through


def block_states(grad4, inputs4, bmat, cmat, enter, leave):
    shape = grad4.shape
    xo = (leave.reshape(shape[0], shape[1], shape[2])[..., None] * inputs4).astype(jnp.bfloat16)
    gi = (enter.reshape(shape[0], shape[1], shape[2])[..., None] * grad4).astype(jnp.bfloat16)
    state = mix("tgkp,tgn->gkpn", xo, bmat)
    adjoint = mix("tgkp,tgn->gkpn", gi, cmat)
    return xo, gi, state, adjoint


def block_grads(grad4, inputs4, bmat, cmat, kernel, leave, xo, gi, entering_state, later, skip):
    length, groups, per_group, head_dim = grad4.shape
    kernel4 = kernel.reshape(length, length, groups, per_group)
    prod = mix("tgkp,ugkp->tugk", grad4, inputs4)
    w_one = (prod * kernel4).astype(jnp.bfloat16)
    cross = mix("tgn,ugn->tug", bmat, cmat)
    w_two = (jnp.swapaxes(kernel4, 0, 1) * cross[:, :, :, None]).astype(jnp.bfloat16)
    grad_c = mix("tugk,ugn->tgn", w_one, bmat) + mix("tgkp,gkpn->tgn", gi, entering_state)
    grad_b = mix("utgk,ugn->tgn", w_one, cmat) + mix("tgkp,gkpn->tgn", xo, later)
    leave4 = leave.reshape(length, groups, per_group)[..., None]
    grad_x = mix("tugk,ugkp->tgkp", w_two, grad4) + leave4 * mix("tgn,gkpn->tgkp", bmat, later)
    grad_x = grad_x + skip.reshape(groups, per_group)[None, :, :, None] * grad4.astype(jnp.float32)
    return grad_x, grad_b, grad_c


def section_backward(incoming, inputs_here, bmat_here, cmat_here, step_here, seg_here, rate, skip, groups, per_group):
    tokens = incoming.shape[0]
    heads = groups * per_group
    head_dim = incoming.shape[1] // heads
    blocks = tokens // BLOCK
    grads = incoming.reshape(blocks, BLOCK, groups, per_group, head_dim)
    inputs = inputs_here.reshape(blocks, BLOCK, groups, per_group, head_dim)
    bmats = bmat_here.reshape(blocks, BLOCK, groups, STATE)
    cmats = cmat_here.reshape(blocks, BLOCK, groups, STATE)
    segs = seg_here.reshape(blocks, BLOCK).astype(jnp.int32)
    prevs = jnp.concatenate([jnp.full((1,), -1, jnp.int32), segs[:-1, -1].astype(jnp.int32)])
    step_blocks = step_here.reshape(blocks, BLOCK, heads)

    def first_pass(item):
        seg, prev, steps_here, grad4, inputs4, bmat, cmat = item
        kernel, enter, leave, through = prepare(seg, prev, steps_here, rate)
        xo, gi, state, adjoint = block_states(grad4, inputs4, bmat, cmat, enter, leave)
        return through.reshape(groups, per_group), state, adjoint

    items = (segs, prevs, step_blocks, grads, inputs, bmats, cmats)
    through, states, adjoints = lax.map(first_pass, items)
    zeros = jnp.zeros((groups, per_group, head_dim, STATE), jnp.float32)

    def forward(carry, item):
        return carry * item[0][:, :, None, None] + item[1], carry

    def backward(carry, item):
        return item[1] + item[0][:, :, None, None] * carry, carry

    unused_one, entering_state = lax.scan(forward, zeros, (through, states))
    unused_two, later = lax.scan(backward, zeros, (through, adjoints), reverse=True)
    entering_state = entering_state.astype(jnp.bfloat16)
    later = later.astype(jnp.bfloat16)

    def second_pass(item):
        seg, prev, steps_here, grad4, inputs4, bmat, cmat, enter_state, later_state = item
        kernel, enter, leave, discarded_result = prepare(seg, prev, steps_here, rate)
        xo, gi, state, adjoint = block_states(grad4, inputs4, bmat, cmat, enter, leave)
        return block_grads(grad4, inputs4, bmat, cmat, kernel, leave, xo, gi, enter_state, later_state, skip)

    grad_x, grad_b, grad_c = lax.map(second_pass, items + (entering_state, later))
    return grad_x.reshape(tokens, heads * head_dim), grad_b.reshape(tokens, groups * STATE), grad_c.reshape(tokens, groups * STATE)


def reference(previous, saved_head_inputs, input_b, input_c, steps, decay_rate, skip_gain, segment_ids, advantage_mask):
    sections = previous.shape[0]
    tokens = previous.shape[1]
    heads = decay_rate.shape[1]
    head_dim = previous.shape[2] // heads
    groups = input_b.shape[2] // STATE
    per_group = heads // groups
    out_x, out_b, out_c, out_skip = [], [], [], []
    for section in range(sections):
        if section == sections - 1:
            incoming = previous[section] * advantage_mask.astype(jnp.bfloat16)[:, None]
        else:
            incoming = previous[section + 1]
        grad_x, grad_b, grad_c = section_backward(incoming, saved_head_inputs[section], input_b[section], input_c[section], steps[section], segment_ids[section], decay_rate[section], skip_gain[section], groups, per_group)
        out_x.append(grad_x.astype(jnp.bfloat16))
        out_b.append(grad_b.astype(jnp.bfloat16))
        out_c.append(grad_c.astype(jnp.bfloat16))
        out_skip.append(mix("thp,thp->h", incoming.reshape(tokens, heads, head_dim), saved_head_inputs[section].reshape(tokens, heads, head_dim)))
    return jnp.stack(out_x), jnp.stack(out_b), jnp.stack(out_c), jnp.stack(out_skip)
```

```python
import jax
import jax.numpy as jnp
from jax import lax
from jax.experimental import pallas as pl
from jax.experimental.pallas import tpu as pltpu
from jax.sharding import Mesh
from jax.sharding import PartitionSpec as P

SEQ = ("seq_0", "seq_1", "seq_2")
MESH = pl.DeviceIdType.MESH
F32 = jnp.float32
BF16 = jnp.bfloat16
NY = 4
T = 128
N = 128
H = 128
D = 64
GROUPS = 8
PAIRS = GROUPS // 2
QL = 256
QUARTERS = 32


def split(v, parts):
    out = []
    for _ in range(parts):
        piece = v.astype(BF16)
        out.append(piece)
        v = v - piece.astype(F32)
    return out


def dot(a, b):
    return lax.dot_general(a, b, (((1,), (0,)), ((), ())), preferred_element_type=F32)


def dot_nt(a, b):
    return lax.dot_general(a, b, (((1,), (1,)), ((), ())), preferred_element_type=F32)


def lanes_of(index, width):
    return pl.ds(pl.multiple_of(index * width, width), width)


def indicator(q, copies):
    row = lax.broadcasted_iota(jnp.int32, (H, QL), 0)
    col = lax.broadcasted_iota(jnp.int32, (H, QL), 1)
    one = jnp.where(row == 4 * q + lax.shift_right_logical(col, 6), 1.0, 0.0).astype(BF16)
    return jnp.concatenate([one] * copies, axis=0)


def make_kernel(nx, nz):
    def kernel(
        prev_ref, x_ref, b_ref, c_ref, steps_ref, rate_ref, skip_ref, seg_ref, mask_ref,
        gx_out, gb_out, gc_out, sk_out,
        grad, xo, gi, gxa, lexp, gca, gba, cum_s, cumt_s, bias_s, biast_s, lvs, ens, bt, ct,
        info_s, info_r, th_s, thx,
        st, sp, tt, tr, zs, zr, es, er, keep, epart, ex, tz_s,
        skp, sk_s, sk_r, skz_s, skz_r,
        gsend, grecv, isend, irecv, ssend, srecv, zsend, zrecv,
        dsend, drecv, tsend, trecv, csend, crecv, esend, erecv, psend, precv,
    ):
        px = lax.axis_index("pipe")
        z = lax.axis_index("seq_0")
        y = lax.axis_index("seq_1")
        c = lax.axis_index("seq_2")
        d = 2 * y + c

        def remote(src, dst, ssem, rsem, where):
            return pltpu.make_async_remote_copy(
                src_ref=src, dst_ref=dst, send_sem=ssem, recv_sem=rsem, device_id=where, device_id_type=MESH
            )

        def grad_copy(k):
            part = lanes_of(k, 2048)
            return remote(
                prev_ref.at[:, part], grad.at[:, part], gsend.at[k], grecv.at[k], (lax.rem(px + nx - 1, nx), z, y, c)
            )

        @pl.when(px > 0)
        def _():
            for k in range(PAIRS):
                grad_copy(k).start()

        row = lax.broadcasted_iota(jnp.int32, (T, T), 0)
        col = lax.broadcasted_iota(jnp.int32, (T, T), 1)
        cum = -(steps_ref[...] * rate_ref[...])
        for shift in (1, 2, 4, 8, 16, 32, 64):
            cum = cum + jnp.where(row >= shift, pltpu.roll(cum, shift, 0), 0.0)
        cum_s[...] = cum
        cumt_s[...] = cum.T
        last = cum[T - 1 : T, :]
        segrow = jnp.broadcast_to(seg_ref[...].astype(F32), (T, T))
        segcol = segrow.T
        seglast = segcol[T - 1 : T, :]
        info_s[0:1, :] = last
        info_s[1:2, :] = seglast
        info_s[2:8, :] = jnp.zeros((6, H), F32)
        info_r[d] = info_s[...]

        def plane_peer(off):
            other = lax.rem(d + off, 2 * NY)
            return (px, z, lax.div(other, 2), lax.rem(other, 2))

        def info_copy(off):
            return remote(info_s, info_r.at[d], isend.at[off - 1], irecv.at[off - 1], plane_peer(off))

        def info_next(other):
            return remote(
                info_s, info_r.at[2 * NY], isend.at[7 + other], irecv.at[7], (px, lax.rem(z + 1, nz), other // 2, other % 2)
            )

        for off in range(1, 2 * NY):
            info_copy(off).start()

        @pl.when((d == 2 * NY - 1) & (z < nz - 1))
        def _():
            for other in range(2 * NY):
                info_next(other).start()

        @pl.when(z == 0)
        def _():
            info_r[2 * NY] = jnp.full((8, H), -1.0, F32)

        linked = segcol == segrow
        bias_s[...] = jnp.where(linked & (row >= col), 0.0, -1e30)
        biast_s[...] = jnp.where(linked & (col >= row), 0.0, -1e30)
        leave = jnp.exp(last - cum) * jnp.where(segcol == seglast, 1.0, 0.0)
        lvs[...] = jnp.concatenate(split(leave, 2), axis=1)

        for g in range(GROUPS):
            part = slice(N * g, N * g + N)
            bt[g] = b_ref[:, part].astype(F32).T.astype(BF16)
            ct[g] = c_ref[:, part].astype(F32).T.astype(BF16)

        mine = c
        theirs = 1 - c

        def partner_copy(w, k):
            return remote(
                st.at[w, 2 * k + theirs], sp.at[w, k], dsend.at[w, k], drecv.at[w, k], (px, z, y, 1 - c)
            )

        def states(w, k, g):
            for s in range(4):
                q = 4 * g + s
                part = lanes_of(q, QL)
                both = indicator(q, 2)
                if w == 0:
                    factor = dot(lvs[...], both)
                    lexp[q] = factor
                    moved = (factor * x_ref[:, part].astype(F32)).astype(BF16)
                    xo[q] = moved
                    st[w, g, s] = dot(bt[g], moved).astype(BF16)
                else:
                    factor = dot(ens[...], both)
                    gr = grad[:, part].astype(F32)
                    moved = (factor * gr).astype(BF16)
                    gi[q] = moved
                    st[w, g, s] = dot(ct[g], moved).astype(BF16)
                    skp[q] = jnp.sum(gr * x_ref[:, part].astype(F32), axis=0, keepdims=True)

        def t_copy(w, k, off):
            other = lax.rem(y + off, NY)
            return remote(
                tt.at[w, k, other], tr.at[w, k, y], tsend.at[w, k, off - 1], trecv.at[w, k, off - 1], (px, z, other, c)
            )

        def chip_state(w, k):
            up, down = (0, 1) if w == 0 else (1, 0)
            partner_copy(w, k).wait_recv()
            g = 2 * k + mine
            for s in range(4):
                own = st[w, g, s].astype(F32)
                other = sp[w, k, s].astype(F32)
                first = jnp.where(c == up, own, other)
                second = jnp.where(c == up, other, own)
                decay = thx[g, s, pl.ds(2 * y + down, 1), :]
                tt[w, k, s] = (decay * first + second).astype(BF16)
            for off in range(1, NY):
                t_copy(w, k, off).start()
            tr[w, k, y] = tt[w, k, y]

        def chain_copy(w, k):
            step = 1 if w == 0 else nz - 1
            return remote(
                zs.at[w, k], zr.at[w, k], csend.at[w, k], crecv.at[w, k], (px, lax.rem(z + step, nz), y, c)
            )

        def e_copy(w, k, off):
            other = lax.rem(y + off, NY)
            return remote(
                es.at[w, k, other], er.at[w, k, y], esend.at[w, k, off - 1], erecv.at[w, k, off - 1], (px, z, other, c)
            )

        def chain(w, k):
            order = tuple(range(NY)) if w == 0 else tuple(reversed(range(NY)))
            first, final = (0, nz - 1) if w == 0 else (nz - 1, 0)
            g = 2 * k + mine
            for off in range(1, NY):
                t_copy(w, k, off).wait_recv()
            decay = [thx[g, y, 2 * i : 2 * i + 1, :] * thx[g, y, 2 * i + 1 : 2 * i + 2, :] for i in range(NY)]
            total = tr[w, k, order[0]].astype(F32)
            factor = decay[order[0]]
            for i in order[1:]:
                total = decay[i] * total + tr[w, k, i].astype(F32)
                factor = factor * decay[i]
            tz_s[...] = total

            @pl.when(z == first)
            def _():
                zr[w, k] = jnp.zeros((N, QL), BF16)

            @pl.when(z != first)
            def _():
                chain_copy(w, k).wait_recv()

            @pl.when(z != final)
            def _():
                zs[w, k] = (factor * zr[w, k].astype(F32) + tz_s[...]).astype(BF16)
                chain_copy(w, k).start()

            value = zr[w, k].astype(F32)
            for i in order:
                es[w, k, i] = value.astype(BF16)
                value = decay[i] * value + tr[w, k, i].astype(F32)
            for off in range(1, NY):
                e_copy(w, k, off).start()
            er[w, k, y] = es[w, k, y]

        def back_copy(w, k):
            return remote(epart.at[w, k], ex.at[w, k], psend.at[w, k], precv.at[w, k], (px, z, y, 1 - c))

        def hand_back(w, k):
            up = 0 if w == 0 else 1
            g = 2 * k + mine
            for off in range(1, NY):
                e_copy(w, k, off).wait_recv()
            for s in range(4):
                here = er[w, k, s]
                first = jnp.where(c == up, st[w, g, s].astype(F32), sp[w, k, s].astype(F32))
                decay = thx[g, s, pl.ds(2 * y + up, 1), :]
                after = decay * here.astype(F32) + first
                keep[w, k, s] = jnp.where(c == up, here.astype(F32), after).astype(BF16)
                epart[w, k, s] = jnp.where(c == up, after, here.astype(F32)).astype(BF16)
            back_copy(w, k).start()

        def fwd_states(k, carry):
            states(0, k, 2 * k + theirs)
            partner_copy(0, k).start()
            states(0, k, 2 * k + mine)
            return carry

        lax.fori_loop(0, PAIRS, fwd_states, 0)

        for off in range(1, 2 * NY):
            info_copy(off).wait_recv()

        @pl.when(z > 0)
        def _():
            remote(
                info_s, info_r.at[2 * NY], isend.at[7], irecv.at[7], (px, lax.rem(z + nz - 1, nz), y, c)
            ).wait_recv()

        th_s[...] = jnp.zeros((16, H), F32)
        for i in range(2 * NY):
            before = info_r[2 * NY if i == 0 else i - 1, 1:2, :]
            th_s[i : i + 1, :] = jnp.exp(info_r[i, 0:1, :]) * jnp.where(info_r[i, 1:2, :] == before, 1.0, 0.0)
        th_s[8:9, :] = skip_ref[...]
        enter_from = info_r[lax.rem(d + 2 * NY, 2 * NY + 1), 1:2, :]
        segc = jnp.broadcast_to(seg_ref[...].astype(F32), (T, T)).T
        enter = jnp.exp(cum_s[...]) * jnp.where(segc == enter_from, 1.0, 0.0)
        ens[...] = jnp.concatenate(split(enter, 2), axis=1)

        def table(g, carry):
            rows = jnp.concatenate(split(th_s[...], 3), axis=1)
            for s in range(4):
                thx[g, s] = dot(rows, indicator(4 * g + s, 3))
            return carry

        lax.fori_loop(0, GROUPS, table, 0)

        def fwd_chip(k, carry):
            chip_state(0, k)
            return carry

        lax.fori_loop(0, PAIRS, fwd_chip, 0)

        @pl.when(px == nx - 1)
        def _():
            keep_rows = jnp.broadcast_to(mask_ref[...].astype(F32), (T, T)).T
            wide = jnp.concatenate([keep_rows, keep_rows], axis=1)

            def body(q, carry):
                part = lanes_of(q, QL)
                grad[:, part] = (prev_ref[:, part].astype(F32) * wide).astype(BF16)
                return carry

            lax.fori_loop(0, QUARTERS, body, 0)

        def within(g):
            bg = b_ref[:, lanes_of(g, N)]
            cg = c_ref[:, lanes_of(g, N)]
            cross = dot_nt(bg, cg)
            cols = pltpu.roll(cum_s[...], lax.rem(H - 16 * g, H), 1)
            low = lax.broadcasted_iota(jnp.int32, (T, T), 1) < D
            total = jnp.zeros((T, T), F32)
            for j in range(8):
                part = pl.ds(pl.multiple_of(1024 * g + 128 * j, 128), 128)
                gp = grad[:, part]
                xp = x_ref[:, part]
                gf = gp.astype(F32)
                both = jnp.concatenate(
                    [jnp.where(low, gf, 0.0).astype(BF16), jnp.where(low, 0.0, gf).astype(BF16)], axis=0
                )
                prod = dot_nt(both, xp)
                pieces = []
                for i in range(2):
                    j2 = 2 * j + i
                    spread = cols[:, j2 : j2 + 1] - cumt_s[pl.ds(16 * g + j2, 1), :]
                    total = total + jnp.exp(spread + bias_s[...]) * prod[T * i : T * i + T, :]
                    pieces.append((jnp.exp(biast_s[...] - spread) * cross).astype(BF16))
                out = dot(jnp.concatenate(pieces, axis=1), both)
                half = slice(128 * (j % 2), 128 * (j % 2) + 128)
                gain = thx[g, j // 2, 8:9, half]
                gxa[4 * g + j // 2, :, half] = out + gain * gf
            gca[g] = dot(total.astype(BF16), bg)
            gba[g] = dot(total.T.astype(BF16), cg)

        def chains(w):
            def body(k, carry):
                chain(w, k)
                return carry

            lax.fori_loop(0, PAIRS, body, 0)

        def main(k, carry):
            @pl.when((k == 1) & (z < nz // 2))
            def _():
                chains(0)

            @pl.when((k == 2) & (z >= nz // 2))
            def _():
                chains(0)

            @pl.when(px < nx - 1)
            def _():
                grad_copy(k).wait_recv()

            states(1, k, 2 * k + theirs)
            partner_copy(1, k).start()
            states(1, k, 2 * k + mine)
            chip_state(1, k)
            within(2 * k)
            within(2 * k + 1)
            return carry

        lax.fori_loop(0, PAIRS, main, 0)

        row_q = lax.broadcasted_iota(jnp.int32, (QL, 128), 0)
        col_q = lax.broadcasted_iota(jnp.int32, (QL, 128), 1)
        pick = jnp.where(lax.shift_right_logical(row_q, 6) == col_q, 1.0, 0.0).astype(BF16)
        sums = jnp.reshape(skp[...], (QUARTERS, QL))
        sk_s[...] = sum(dot(piece, pick) for piece in split(sums, 3))
        sk_r[d] = sk_s[...]

        def sk_copy(off):
            return remote(sk_s, sk_r.at[d], ssend.at[off - 1], srecv.at[off - 1], plane_peer(off))

        def skz_copy(off):
            return remote(
                skz_s, skz_r.at[z], zsend.at[off - 1], zrecv.at[off - 1], (px, lax.rem(z + off, nz), y, c)
            )

        for off in range(1, 2 * NY):
            sk_copy(off).start()

        def fwd_back(k, carry):
            hand_back(0, k)
            return carry

        lax.fori_loop(0, PAIRS, fwd_back, 0)

        def finish_c(g, source, k):
            acc = gca[g]
            for s in range(4):
                acc = acc + dot_nt(gi[4 * g + s], source[0, k, s])
            gc_out[:, lanes_of(g, N)] = acc.astype(BF16)

        def finish_b(g, source, k):
            acc = gba[g]
            bg = b_ref[:, lanes_of(g, N)]
            for s in range(4):
                q = 4 * g + s
                later = source[1, k, s]
                acc = acc + dot_nt(xo[q], later)
                gx_out[:, lanes_of(q, QL)] = (gxa[q] + lexp[q] * dot(bg, later)).astype(BF16)
            gb_out[:, lanes_of(g, N)] = acc.astype(BF16)

        def end_c(k, carry):
            finish_c(2 * k + mine, keep, k)
            back_copy(0, k).wait_recv()
            finish_c(2 * k + theirs, ex, k)
            return carry

        chains(1)
        lax.fori_loop(0, PAIRS, end_c, 0)

        for off in range(1, 2 * NY):
            sk_copy(off).wait_recv()
        acc = sk_r[0]
        for i in range(1, 2 * NY):
            acc = acc + sk_r[i]
        skz_s[...] = acc
        skz_r[z] = acc
        for off in range(1, nz):
            skz_copy(off).start()

        def bwd_back(k, carry):
            hand_back(1, k)
            finish_b(2 * k + mine, keep, k)
            return carry

        lax.fori_loop(0, PAIRS, bwd_back, 0)

        def end_b(k, carry):
            back_copy(1, k).wait_recv()
            finish_b(2 * k + theirs, ex, k)
            return carry

        lax.fori_loop(0, PAIRS, end_b, 0)

        for off in range(1, nz):
            skz_copy(off).wait_recv()
        acc = skz_r[0]
        for i in range(1, nz):
            acc = acc + skz_r[i]
        sk_out[...] = acc

        @pl.when(px > 0)
        def _():
            for k in range(PAIRS):
                grad_copy(k).wait_send()

        for off in range(1, 2 * NY):
            info_copy(off).wait_send()
            sk_copy(off).wait_send()

        @pl.when((d == 2 * NY - 1) & (z < nz - 1))
        def _():
            for other in range(2 * NY):
                info_next(other).wait_send()

        for off in range(1, nz):
            skz_copy(off).wait_send()

        for w in range(2):
            final = nz - 1 if w == 0 else 0

            def drain(k, carry, w=w, final=final):
                partner_copy(w, k).wait_send()
                back_copy(w, k).wait_send()
                for off in range(1, NY):
                    t_copy(w, k, off).wait_send()
                    e_copy(w, k, off).wait_send()

                @pl.when(z != final)
                def _():
                    chain_copy(w, k).wait_send()

                return carry

            lax.fori_loop(0, PAIRS, drain, 0)

    return kernel


def call(nx, nz):
    vm = pltpu.VMEM
    dma = pltpu.SemaphoreType.DMA
    scratch = [
        vm((T, H * D), BF16),
        vm((QUARTERS, T, QL), BF16),
        vm((QUARTERS, T, QL), BF16),
        vm((QUARTERS, T, QL), F32),
        vm((QUARTERS, T, QL), F32),
        vm((GROUPS, T, N), F32),
        vm((GROUPS, T, N), F32),
        vm((T, H), F32),
        vm((H, T), F32),
        vm((T, T), F32),
        vm((T, T), F32),
        vm((T, 2 * H), BF16),
        vm((T, 2 * H), BF16),
        vm((GROUPS, N, T), BF16),
        vm((GROUPS, N, T), BF16),
        vm((8, H), F32),
        vm((2 * NY + 1, 8, H), F32),
        vm((16, H), F32),
        vm((GROUPS, 4, 16, QL), F32),
        vm((2, GROUPS, 4, N, QL), BF16),
        vm((2, PAIRS, 4, N, QL), BF16),
        vm((2, PAIRS, NY, N, QL), BF16),
        vm((2, PAIRS, NY, N, QL), BF16),
        vm((2, PAIRS, N, QL), BF16),
        vm((2, PAIRS, N, QL), BF16),
        vm((2, PAIRS, NY, N, QL), BF16),
        vm((2, PAIRS, NY, N, QL), BF16),
        vm((2, PAIRS, 4, N, QL), BF16),
        vm((2, PAIRS, 4, N, QL), BF16),
        vm((2, PAIRS, 4, N, QL), BF16),
        vm((N, QL), F32),
        vm((QUARTERS, 1, QL), F32),
        vm((QUARTERS, 128), F32),
        vm((2 * NY, QUARTERS, 128), F32),
        vm((QUARTERS, 128), F32),
        vm((nz, QUARTERS, 128), F32),
        dma((PAIRS,)), dma((PAIRS,)),
        dma((7 + 2 * NY,)), dma((8,)),
        dma((7,)), dma((7,)),
        dma((nz - 1,)), dma((nz - 1,)),
        dma((2, PAIRS)), dma((2, PAIRS)),
        dma((2, PAIRS, NY - 1)), dma((2, PAIRS, NY - 1)),
        dma((2, PAIRS)), dma((2, PAIRS)),
        dma((2, PAIRS, NY - 1)), dma((2, PAIRS, NY - 1)),
        dma((2, PAIRS)), dma((2, PAIRS)),
    ]
    return pl.pallas_call(
        make_kernel(nx, nz),
        out_shape=(
            jax.ShapeDtypeStruct((T, H * D), BF16),
            jax.ShapeDtypeStruct((T, GROUPS * N), BF16),
            jax.ShapeDtypeStruct((T, GROUPS * N), BF16),
            jax.ShapeDtypeStruct((QUARTERS, 128), F32),
        ),
        in_specs=[pl.BlockSpec(memory_space=pltpu.VMEM)] * 9,
        out_specs=[pl.BlockSpec(memory_space=pltpu.VMEM)] * 4,
        scratch_shapes=scratch,
        compiler_params=pltpu.CompilerParams(vmem_limit_bytes=62 * 2**20),
        name="mixer_backward",
    )


def on_device(previous, saved_head_inputs, input_b, input_c, steps, decay_rate, skip_gain, segment_ids, advantage_mask):
    kernel = call(lax.axis_size("pipe"), lax.axis_size("seq_0"))
    gx, gb, gc, sk = kernel(
        previous[0],
        saved_head_inputs[0],
        input_b[0],
        input_c[0],
        steps[0],
        decay_rate,
        skip_gain,
        segment_ids,
        advantage_mask[None],
    )
    return gx[None], gb[None], gc[None], sk[:, :4].reshape(1, H)


def solution(mesh):
    finer = Mesh(
        mesh.devices.reshape(mesh.shape["pipe"], mesh.shape["seq"] // (2 * NY), NY, 2),
        ("pipe", "seq_0", "seq_1", "seq_2"),
    )
    return jax.shard_map(
        on_device,
        mesh=finer,
        in_specs=(
            P("pipe", SEQ, None),
            P("pipe", SEQ, None),
            P("pipe", SEQ, None),
            P("pipe", SEQ, None),
            P("pipe", SEQ, None),
            P("pipe", None),
            P("pipe", None),
            P("pipe", SEQ),
            P(SEQ),
        ),
        out_specs=(
            P("pipe", SEQ, None),
            P("pipe", SEQ, None),
            P("pipe", SEQ, None),
            P("pipe", None),
        ),
        check_vma=False,
    )
```

```python
import jax
import jax.numpy as jnp
from jax import lax
from jax.experimental import pallas as pl
from jax.experimental.pallas import tpu as pltpu
from jax.sharding import Mesh
from jax.sharding import PartitionSpec as P

SEQ = ("seq_0", "seq_1", "seq_2")
MESH = pl.DeviceIdType.MESH
F32 = jnp.float32
BF16 = jnp.bfloat16
NY = 4
T = 128
N = 128
H = 128
D = 64
GROUPS = 8
CHUNKS = 8
MINE = 2 * CHUNKS
ROWS = N // NY
QL = 256
QUARTERS = 32


def split(v, parts):
    out = []
    for _ in range(parts):
        piece = v.astype(BF16)
        out.append(piece)
        v = v - piece.astype(F32)
    return out


def dot(a, b):
    return lax.dot_general(a, b, (((1,), (0,)), ((), ())), preferred_element_type=F32)


def dot_nt(a, b):
    return lax.dot_general(a, b, (((1,), (1,)), ((), ())), preferred_element_type=F32)


def lanes_of(index, width):
    return pl.ds(pl.multiple_of(index * width, width), width)


def indicator(q, copies):
    row = lax.broadcasted_iota(jnp.int32, (H, QL), 0)
    col = lax.broadcasted_iota(jnp.int32, (H, QL), 1)
    one = jnp.where(row == 4 * q + lax.shift_right_logical(col, 6), 1.0, 0.0).astype(BF16)
    return jnp.concatenate([one] * copies, axis=0)


def make_kernel(nx, nz):
    width = (4, 2)
    count = (MINE // 4, CHUNKS)

    def kernel(
        prev_ref, x_ref, b_ref, c_ref, steps_ref, rate_ref, skip_ref, seg_ref, mask_ref,
        gx_out, gb_out, gc_out, sk_out,
        grad, xo, gi, gxa, lexp, gca, gba, cum_s, cumt_s, bias_s, biast_s, eexp, lvs, bt, ct, wide_s, fz_s, fz_r, fzx,
        info_s, info_r, th_s, thx,
        st, sp, tt, t1, us, u2, zs, zr, az, ho, hi, vo, vi, eo, er, keep, epart, ex, tz_s,
        skp, sk_s, sk_r, skz_s, skz_r,
        gsend, grecv, isend, irecv, ssend, srecv, zsend, zrecv,
        fsend, frecv, asend, arecv, hsend, hrecv, dsend, drecv, t1send, t1recv, u2send, u2recv, csend, crecv, v2send, v2recv, e1send, e1recv, psend, precv,
    ):
        px = lax.axis_index("pipe")
        z = lax.axis_index("seq_0")
        y = lax.axis_index("seq_1")
        c = lax.axis_index("seq_2")
        d = 2 * y + c
        last_d = 2 * NY - 1

        def remote(src, dst, ssem, rsem, where):
            return pltpu.make_async_remote_copy(
                src_ref=src, dst_ref=dst, send_sem=ssem, recv_sem=rsem, device_id=where, device_id_type=MESH
            )

        def plane_peer(off):
            other = lax.rem(d + off, 2 * NY)
            return (px, z, lax.div(other, 2), lax.rem(other, 2))

        def z_peer(off):
            return (px, lax.rem(z + off, nz), y, c)

        barrier = pltpu.get_barrier_semaphore()

        def greet(where):
            pl.semaphore_signal(barrier, inc=1, device_id=where, device_id_type=MESH)

        for off in range(1, 2 * NY):
            greet(plane_peer(off))
        for off in range(1, nz):
            greet(z_peer(off))

        @pl.when(px < nx - 1)
        def _():
            greet((lax.rem(px + 1, nx), z, y, c))

        @pl.when(z > 0)
        def _():
            greet((px, lax.rem(z + nz - 1, nz), NY - 1, 1))

        from_next = (d == last_d) & (z < nz - 1)
        callers = 2 * NY - 1 + nz - 1 + jnp.where(px > 0, 1, 0) + jnp.where(from_next, 2 * NY, 0)
        pl.semaphore_wait(barrier, callers)

        def grad_copy(k):
            part = lanes_of(k, 4 * QL)
            return remote(
                prev_ref.at[:, part], grad.at[:, part], gsend.at[k], grecv.at[k], (lax.rem(px + nx - 1, nx), z, y, c)
            )

        @pl.when(px > 0)
        def _():
            def body(k, carry):
                grad_copy(k).start()
                return carry

            lax.fori_loop(0, CHUNKS, body, 0)

        row = lax.broadcasted_iota(jnp.int32, (T, T), 0)
        col = lax.broadcasted_iota(jnp.int32, (T, T), 1)
        cum = -(steps_ref[...] * rate_ref[...])
        for shift in (1, 2, 4, 8, 16, 32, 64):
            cum = cum + jnp.where(row >= shift, pltpu.roll(cum, shift, 0), 0.0)
        cum_s[...] = cum
        cumt_s[...] = cum.T
        last = cum[T - 1 : T, :]
        segrow = jnp.broadcast_to(seg_ref[...].astype(F32), (T, T))
        segcol = segrow.T
        seglast = segcol[T - 1 : T, :]
        info_s[0:1, :] = last
        info_s[1:2, :] = seglast
        info_s[2:8, :] = jnp.zeros((6, H), F32)
        info_r[d] = info_s[...]

        def info_copy(off):
            return remote(info_s, info_r.at[d], isend.at[off - 1], irecv.at[off - 1], plane_peer(off))

        def info_next(other):
            return remote(
                info_s, info_r.at[2 * NY], isend.at[7 + other], irecv.at[7], (px, lax.rem(z + 1, nz), other // 2, other % 2)
            )

        for off in range(1, 2 * NY):
            info_copy(off).start()

        @pl.when((d == last_d) & (z < nz - 1))
        def _():
            for other in range(2 * NY):
                info_next(other).start()

        @pl.when(z == 0)
        def _():
            info_r[2 * NY] = jnp.full((8, H), -1.0, F32)

        linked = segcol == segrow
        bias_s[...] = jnp.where(linked & (row >= col), 0.0, -1e30)
        biast_s[...] = jnp.where(linked & (col >= row), 0.0, -1e30)
        leave = jnp.exp(last - cum) * jnp.where(segcol == seglast, 1.0, 0.0)
        lvs[...] = jnp.concatenate(split(leave, 2), axis=1)
        kept = jnp.broadcast_to(mask_ref[...].astype(F32), (T, T)).T
        wide_s[...] = jnp.concatenate([kept, kept], axis=1)

        for g in range(GROUPS):
            part = slice(N * g, N * g + N)
            bt[g] = b_ref[:, part].astype(F32).T.astype(BF16)
            ct[g] = c_ref[:, part].astype(F32).T.astype(BF16)

        pair = lax.div(y, 2)
        low_y = lax.rem(y, 2)
        half_of = jnp.where(low_y == pair, 0, 1)
        in_pair = (px, z, 2 * pair + 1 - low_y, c)
        over_pairs = (px, z, NY - 1 - y, c)

        mine = c
        theirs = 1 - c

        def some(ref, w, k):
            return ref.at[w, pl.ds(width[w] * k, width[w])]

        def partner_copy(w, k):
            n = width[w]
            return remote(
                st.at[w, theirs, pl.ds(n * k, n)], some(sp, w, k), dsend.at[w, k], drecv.at[w, k], (px, z, y, 1 - c)
            )

        def quarter(m, side):
            return 4 * lax.div(m, 2) + 2 * side + lax.rem(m, 2)

        def states(w, k, side):
            for i in range(width[w]):
                m = width[w] * k + i
                q = quarter(m, side)
                g = lax.div(m, 2)
                part = lanes_of(q, QL)
                if w == 0:
                    factor = dot(lvs[...], indicator(q, 2))
                    lexp[q] = factor
                    moved = (factor * x_ref[:, part].astype(F32)).astype(BF16)
                    xo[q] = moved
                    st[w, side, m] = dot(bt[g], moved).astype(BF16)
                else:
                    gr = grad[:, part].astype(F32)
                    moved = (eexp[q] * gr).astype(BF16)
                    gi[q] = moved
                    st[w, side, m] = dot(ct[g], moved).astype(BF16)
                    skp[q] = jnp.sum(gr * x_ref[:, part].astype(F32), axis=0, keepdims=True)

        def t_copy(w, k):
            m = pl.ds(width[w] * k, width[w])
            return remote(tt.at[w, m, 1 - half_of], t1.at[w, m], t1send.at[w, k], t1recv.at[w, k], in_pair)

        def u_copy(w, k):
            m = pl.ds(width[w] * k, width[w])
            return remote(us.at[w, m, 1 - pair], u2.at[w, m], u2send.at[w, k], u2recv.at[w, k], over_pairs)

        def v_copy(w, k):
            m = pl.ds(width[w] * k, width[w])
            return remote(vo.at[w, m], vi.at[w, m, pair], v2send.at[w, k], v2recv.at[w, k], over_pairs)

        def e_copy(w, k):
            m = pl.ds(width[w] * k, width[w])
            return remote(eo.at[w, m], er.at[w, m, half_of], e1send.at[w, k], e1recv.at[w, k], in_pair)

        def chip_decay(q, chip):
            return thx[q, pl.ds(2 * chip, 1), :] * thx[q, pl.ds(2 * chip + 1, 1), :]

        def pair_decay(q, which):
            return chip_decay(q, 2 * which) * chip_decay(q, 2 * which + 1)

        def chip_state(w, k):
            up, down = (0, 1) if w == 0 else (1, 0)
            partner_copy(w, k).wait_recv()
            for i in range(width[w]):
                m = width[w] * k + i
                own = st[w, mine, m].astype(F32)
                other = sp[w, m].astype(F32)
                first = jnp.where(c == up, own, other)
                second = jnp.where(c == up, other, own)
                decay = thx[quarter(m, mine), pl.ds(2 * y + down, 1), :]
                tt[w, m] = (decay * first + second).astype(BF16).reshape(2, 2 * ROWS, QL)
            t_copy(w, k).start()

        def pair_first(w, m):
            own = tt[w, m, half_of].astype(F32)
            other = t1[w, m].astype(F32)
            return jnp.where(low_y == w, own, other), jnp.where(low_y == w, other, own)

        def pair_step(w, k):
            t_copy(w, k).wait_recv()
            for i in range(width[w]):
                m = width[w] * k + i
                first, second = pair_first(w, m)
                decay = chip_decay(quarter(m, mine), 2 * pair + 1 - w)
                us[w, m] = (decay * first + second).astype(BF16).reshape(2, ROWS, QL)
            u_copy(w, k).start()

        def plane_first(w, m):
            own = us[w, m, pair].astype(F32)
            other = u2[w, m].astype(F32)
            return jnp.where(pair == w, own, other), jnp.where(pair == w, other, own)

        def chain_copy(k):
            m = pl.ds(width[0] * k, width[0])
            return remote(zs.at[m], zr.at[m], csend.at[k], crecv.at[k], z_peer(1))

        def across(k, other):
            m = pl.ds(width[1] * k, width[1])
            return remote(az.at[z, m], az.at[z, m], asend.at[k, other], arecv.at[k, z], (px, other, y, c))

        half = nz // 2
        start = half * lax.div(z, half)

        def down(k, other):
            m = pl.ds(width[1] * k, width[1])
            return remote(ho.at[m], hi.at[m], hsend.at[k, other], hrecv.at[k], (px, other, y, c))

        def arrived(k, source):
            m = pl.ds(width[1] * k, width[1])
            return remote(az.at[source, m], az.at[source, m], asend.at[k, source], arecv.at[k, source], (px, source, y, c))

        def plane_total(w, m):
            q = quarter(m, mine)
            first, second = plane_first(w, m)
            decay = pair_decay(q, 1 - w)
            return decay * first + second, decay * pair_decay(q, w)

        def spread_out(w, k, values):
            for i, value in enumerate(values):
                m = width[w] * k + i
                after = pair_decay(quarter(m, mine), w) * value + plane_first(w, m)[0]
                vi[w, m, pair] = jnp.where(pair == w, value, after).astype(BF16)
                vo[w, m] = jnp.where(pair == w, after, value).astype(BF16)
            v_copy(w, k).start()

        def pair_out(w, k):
            v_copy(w, k).wait_recv()
            for i in range(width[w]):
                m = width[w] * k + i
                value = vi[w, m].reshape(2 * ROWS, QL).astype(F32)
                after = chip_decay(quarter(m, mine), 2 * pair + w) * value + pair_first(w, m)[0]
                er[w, m, half_of] = jnp.where(low_y == w, value, after).astype(BF16)
                eo[w, m] = jnp.where(low_y == w, after, value).astype(BF16)
            e_copy(w, k).start()

        def chain(k):
            u_copy(0, k).wait_recv()
            held = []
            for i in range(width[0]):
                m = width[0] * k + i
                total, factor = plane_total(0, m)
                tz_s[i] = total
                held.append((m, factor))

            @pl.when(z == 0)
            def _():
                for m, _factor in held:
                    zr[m] = jnp.zeros((ROWS, QL), BF16)

            @pl.when(z > 0)
            def _():
                chain_copy(k).wait_recv()

            @pl.when(z < nz - 1)
            def _():
                for i, (m, factor) in enumerate(held):
                    zs[m] = (factor * zr[m].astype(F32) + tz_s[i]).astype(BF16)
                chain_copy(k).start()

            spread_out(0, k, [zr[m].astype(F32) for m, _factor in held])

        def plane_send(k):
            u_copy(1, k).wait_recv()
            for i in range(width[1]):
                m = width[1] * k + i
                az[z, m] = plane_total(1, m)[0].astype(BF16)

            def body(other, carry):
                across(k, other).start()
                return carry

            lax.fori_loop(start, z, body, 0)

        def plane_back(k):
            @pl.when(z >= half)
            def _():
                for i in range(width[1]):
                    tz_s[i] = jnp.zeros((ROWS, QL), F32)

            @pl.when(z < half)
            def _():
                down(k, half).wait_recv()
                for i in range(width[1]):
                    tz_s[i] = hi[width[1] * k + i].astype(F32)

            def body(t, carry):
                source = start + half - 1 - t
                arrived(k, source).wait_recv()
                for i in range(width[1]):
                    m = width[1] * k + i
                    factor = fzx[quarter(m, mine), pl.ds(source, 1), :]
                    tz_s[i] = factor * tz_s[i] + az[source, m].astype(F32)
                return carry

            lax.fori_loop(0, start + half - 1 - z, body, 0)

            @pl.when(z == half)
            def _():
                for i in range(width[1]):
                    m = width[1] * k + i
                    total, factor = plane_total(1, m)
                    ho[m] = (factor * tz_s[i] + total).astype(BF16)
                for other in range(half):
                    down(k, other).start()

            spread_out(1, k, [tz_s[i] for i in range(width[1])])

        def back_copy(w, k):
            return remote(some(epart, w, k), some(ex, w, k), psend.at[w, k], precv.at[w, k], (px, z, y, 1 - c))

        def hand_back(w, k):
            up = 0 if w == 0 else 1
            e_copy(w, k).wait_recv()
            for i in range(width[w]):
                m = width[w] * k + i
                here = er[w, m].reshape(N, QL).astype(F32)
                first = jnp.where(c == up, st[w, mine, m].astype(F32), sp[w, m].astype(F32))
                decay = thx[quarter(m, mine), pl.ds(2 * y + up, 1), :]
                after = decay * here + first
                keep[w, m] = jnp.where(c == up, here, after).astype(BF16)
                epart[w, m] = jnp.where(c == up, after, here).astype(BF16)
            back_copy(w, k).start()

        def finish_c(k):
            back_copy(0, k).wait_recv()
            for j in range(2):
                g = 2 * k + j
                acc = gca[g]
                for i in range(2):
                    m = 2 * g + i
                    acc = acc + dot_nt(gi[quarter(m, mine)], keep[0, m]) + dot_nt(gi[quarter(m, theirs)], ex[0, m])
                gc_out[:, lanes_of(g, N)] = acc.astype(BF16)

        def finish_b(g):
            back_copy(1, g).wait_recv()
            bg = b_ref[:, lanes_of(g, N)]
            acc = gba[g]
            for side, source in ((mine, keep), (theirs, ex)):
                for i in range(2):
                    m = 2 * g + i
                    q = quarter(m, side)
                    later = source[1, m]
                    acc = acc + dot_nt(xo[q], later)
                    gx_out[:, lanes_of(q, QL)] = (gxa[q] + lexp[q] * dot(bg, later)).astype(BF16)
            gb_out[:, lanes_of(g, N)] = acc.astype(BF16)

        def fwd_states(k, carry):
            states(0, k, theirs)
            partner_copy(0, k).start()
            states(0, k, mine)
            return carry

        lax.fori_loop(0, count[0], fwd_states, 0)

        for off in range(1, 2 * NY):
            info_copy(off).wait_recv()

        @pl.when(z > 0)
        def _():
            remote(info_s, info_r.at[2 * NY], isend.at[7], irecv.at[7], z_peer(nz - 1)).wait_recv()

        th_s[...] = jnp.zeros((16, H), F32)
        for i in range(2 * NY):
            before = info_r[2 * NY if i == 0 else i - 1, 1:2, :]
            th_s[i : i + 1, :] = jnp.exp(info_r[i, 0:1, :]) * jnp.where(info_r[i, 1:2, :] == before, 1.0, 0.0)
        th_s[8:9, :] = skip_ref[...]
        enter_from = info_r[lax.rem(d + 2 * NY, 2 * NY + 1), 1:2, :]
        segc = jnp.broadcast_to(seg_ref[...].astype(F32), (T, T)).T
        enter = jnp.exp(cum_s[...]) * jnp.where(segc == enter_from, 1.0, 0.0)
        lvs[...] = jnp.concatenate(split(enter, 2), axis=1)
        whole = th_s[0:1, :]
        for i in range(1, 2 * NY):
            whole = whole * th_s[i : i + 1, :]
        fz_s[...] = jnp.broadcast_to(whole, (8, H))
        fz_r[z] = fz_s[...]

        def f_copy(other):
            return remote(fz_s, fz_r.at[z], fsend.at[other], frecv.at[z], (px, other, y, c))

        def f_arrived(source):
            return remote(fz_s, fz_r.at[source], fsend.at[source], frecv.at[source], (px, source, y, c))

        def f_start(other, carry):
            f_copy(other).start()
            return carry

        lax.fori_loop(0, z, f_start, 0)

        def table(k, carry):
            rows = jnp.concatenate(split(th_s[...], 3), axis=1)
            for i in range(4):
                thx[4 * k + i] = dot(rows, indicator(4 * k + i, 3))
            return carry

        lax.fori_loop(0, QUARTERS // 4, table, 0)

        def fwd_chip(k, carry):
            chip_state(0, k)
            return carry

        lax.fori_loop(0, count[0], fwd_chip, 0)

        def enter_wide(k, carry):
            for i in range(4):
                eexp[4 * k + i] = dot(lvs[...], indicator(4 * k + i, 2))
            return carry

        enter_wide(0, 0)

        def f_wait(t, carry):
            f_arrived(nz - 1 - t).wait_recv()
            return carry

        def plane_table():
            lax.fori_loop(0, nz - 1 - z, f_wait, 0)
            everything = jnp.concatenate(
                [jnp.where(i > z, fz_r[i, 0:1, :], 0.0) for i in range(nz)], axis=0
            )
            th_s[0:nz, :] = everything

            def body(k, carry):
                rows = jnp.concatenate(split(th_s[...], 3), axis=1)
                for i in range(4):
                    fzx[4 * k + i] = dot(rows, indicator(4 * k + i, 3))
                return carry

            lax.fori_loop(0, QUARTERS // 4, body, 0)

        def within(g):
            bg = b_ref[:, lanes_of(g, N)]
            cg = c_ref[:, lanes_of(g, N)]
            cross = dot_nt(bg, cg)
            cols = pltpu.roll(cum_s[...], lax.rem(H - 16 * g, H), 1)
            low = lax.broadcasted_iota(jnp.int32, (T, T), 1) < D
            total = jnp.zeros((T, T), F32)
            for j in range(8):
                part = pl.ds(pl.multiple_of(1024 * g + 128 * j, 128), 128)
                gf = grad[:, part].astype(F32)
                xp = x_ref[:, part]
                both = jnp.concatenate(
                    [jnp.where(low, gf, 0.0).astype(BF16), jnp.where(low, 0.0, gf).astype(BF16)], axis=0
                )
                prod = dot_nt(both, xp)
                pieces = []
                for i in range(2):
                    j2 = 2 * j + i
                    spread = cols[:, j2 : j2 + 1] - cumt_s[pl.ds(16 * g + j2, 1), :]
                    total = total + jnp.exp(spread + bias_s[...]) * prod[T * i : T * i + T, :]
                    pieces.append((jnp.exp(biast_s[...] - spread) * cross).astype(BF16))
                out = dot(jnp.concatenate(pieces, axis=1), both)
                half = slice(128 * (j % 2), 128 * (j % 2) + 128)
                q = 4 * g + j // 2
                gxa[q, :, half] = out + thx[q, 8:9, half] * gf
            gca[g] = dot(total.astype(BF16), bg)
            gba[g] = dot(total.T.astype(BF16), cg)

        def sk_copy(off):
            return remote(sk_s, sk_r.at[d], ssend.at[off - 1], srecv.at[off - 1], plane_peer(off))

        def skz_copy(off):
            return remote(skz_s, skz_r.at[z], zsend.at[off - 1], zrecv.at[off - 1], z_peer(off))

        def sk_plane():
            row_q = lax.broadcasted_iota(jnp.int32, (QL, 128), 0)
            col_q = lax.broadcasted_iota(jnp.int32, (QL, 128), 1)
            pick = jnp.where(lax.shift_right_logical(row_q, 6) == (col_q & 3), 1.0, 0.0).astype(BF16)
            sums = jnp.reshape(skp[...], (QUARTERS, QL))
            heads = sum(dot(piece, pick) for piece in split(sums, 3))
            own_row = lax.broadcasted_iota(jnp.int32, (QUARTERS, 128), 0)
            own_col = lax.broadcasted_iota(jnp.int32, (QUARTERS, 128), 1)
            heads = jnp.where(lax.shift_right_logical(own_col, 2) == own_row, heads, 0.0)
            sk_s[...] = jnp.broadcast_to(jnp.sum(heads, axis=0, keepdims=True), (8, 128))
            sk_r[d] = sk_s[...]
            for off in range(1, 2 * NY):
                sk_copy(off).start()

        def sk_along():
            for off in range(1, 2 * NY):
                sk_copy(off).wait_recv()
            acc = sk_r[0]
            for i in range(1, 2 * NY):
                acc = acc + sk_r[i]
            skz_s[...] = acc
            skz_r[z] = acc
            for off in range(1, nz):
                skz_copy(off).start()

        def each(n, step):
            def body(k, carry):
                step(k)
                return carry

            lax.fori_loop(0, n, body, 0)

        chain_at = 2 + lax.div(z * 5 + 3, nz - 1)
        back_at = jnp.where(z < half, 4, 3)

        def main(k, carry):
            def at(lag, n, step):
                @pl.when((k >= lag) & (k < lag + n))
                def _():
                    step(k - lag)

            def begin(k):
                @pl.when(px == nx - 1)
                def _():
                    for i in range(4):
                        part = lanes_of(4 * k + i, QL)
                        grad[:, part] = (prev_ref[:, part].astype(F32) * wide_s[...]).astype(BF16)

                @pl.when(px < nx - 1)
                def _():
                    grad_copy(k).wait_recv()

                states(1, k, theirs)
                partner_copy(1, k).start()
                states(1, k, mine)

                @pl.when(k < CHUNKS - 1)
                def _():
                    enter_wide(k + 1, 0)

                chip_state(1, k)
                within(k)

            at(0, CHUNKS, begin)

            @pl.when(k == 1)
            def _():
                plane_table()

            @pl.when(k == CHUNKS)
            def _():
                sk_plane()

            at(1, count[1], lambda i: pair_step(1, i))
            at(2, count[1], plane_send)
            at(back_at, count[1], plane_back)
            at(back_at + 1, count[1], lambda i: pair_out(1, i))
            at(back_at + 2, count[1], lambda i: hand_back(1, i))

            @pl.when(k == CHUNKS + 2)
            def _():
                sk_along()

            at(back_at + 3, count[1], finish_b)
            at(1, count[0], lambda i: pair_step(0, i))
            at(chain_at, count[0], chain)
            at(chain_at + 1, count[0], lambda i: pair_out(0, i))
            at(chain_at + 2, count[0], lambda i: hand_back(0, i))
            at(chain_at + 3, count[0], finish_c)
            return carry

        lax.fori_loop(0, CHUNKS + 7, main, 0)

        for off in range(1, nz):
            skz_copy(off).wait_recv()
        acc = skz_r[0]
        for i in range(1, nz):
            acc = acc + skz_r[i]
        sk_out[...] = acc[0:1, :]

        @pl.when(px > 0)
        def _():
            def body(k, carry):
                grad_copy(k).wait_send()
                return carry

            lax.fori_loop(0, CHUNKS, body, 0)

        for off in range(1, 2 * NY):
            info_copy(off).wait_send()
            sk_copy(off).wait_send()

        @pl.when((d == last_d) & (z < nz - 1))
        def _():
            for other in range(2 * NY):
                info_next(other).wait_send()

        for off in range(1, nz):
            skz_copy(off).wait_send()

        for w in range(2):

            def drain(k, w=w):
                partner_copy(w, k).wait_send()
                back_copy(w, k).wait_send()
                t_copy(w, k).wait_send()
                u_copy(w, k).wait_send()
                v_copy(w, k).wait_send()
                e_copy(w, k).wait_send()
                if w == 0:

                    @pl.when(z < nz - 1)
                    def _():
                        chain_copy(k).wait_send()
                else:

                    def let_go(other, carry, k=k):
                        across(k, other).wait_send()
                        return carry

                    lax.fori_loop(start, z, let_go, 0)

                    @pl.when(z == half)
                    def _():
                        for other in range(half):
                            down(k, other).wait_send()


            each(count[w], drain)
        each(z, lambda other: f_copy(other).wait_send())

    return kernel


def call(nx, nz):
    vm = pltpu.VMEM
    dma = pltpu.SemaphoreType.DMA
    scratch = [
        vm((T, H * D), BF16),
        vm((QUARTERS, T, QL), BF16),
        vm((QUARTERS, T, QL), BF16),
        vm((QUARTERS, T, QL), F32),
        vm((QUARTERS, T, QL), F32),
        vm((GROUPS, T, N), F32),
        vm((GROUPS, T, N), F32),
        vm((T, H), F32),
        vm((H, T), F32),
        vm((T, T), F32),
        vm((T, T), F32),
        vm((QUARTERS, T, QL), F32),
        vm((T, 2 * H), BF16),
        vm((GROUPS, N, T), BF16),
        vm((GROUPS, N, T), BF16),
        vm((T, QL), F32),
        vm((8, H), F32),
        vm((nz, 8, H), F32),
        vm((QUARTERS, 16, QL), F32),
        vm((8, H), F32),
        vm((2 * NY + 1, 8, H), F32),
        vm((16, H), F32),
        vm((QUARTERS, 16, QL), F32),
        vm((2, 2, MINE, N, QL), BF16),
        vm((2, MINE, N, QL), BF16),
        vm((2, MINE, 2, 2 * ROWS, QL), BF16),
        vm((2, MINE, 2 * ROWS, QL), BF16),
        vm((2, MINE, 2, ROWS, QL), BF16),
        vm((2, MINE, ROWS, QL), BF16),
        vm((MINE, ROWS, QL), BF16),
        vm((MINE, ROWS, QL), BF16),
        vm((nz, MINE, ROWS, QL), BF16),
        vm((MINE, ROWS, QL), BF16),
        vm((MINE, ROWS, QL), BF16),
        vm((2, MINE, ROWS, QL), BF16),
        vm((2, MINE, 2, ROWS, QL), BF16),
        vm((2, MINE, 2 * ROWS, QL), BF16),
        vm((2, MINE, 2, 2 * ROWS, QL), BF16),
        vm((2, MINE, N, QL), BF16),
        vm((2, MINE, N, QL), BF16),
        vm((2, MINE, N, QL), BF16),
        vm((4, ROWS, QL), F32),
        vm((QUARTERS, 1, QL), F32),
        vm((8, 128), F32),
        vm((2 * NY, 8, 128), F32),
        vm((8, 128), F32),
        vm((nz, 8, 128), F32),
        dma((CHUNKS,)), dma((CHUNKS,)),
        dma((7 + 2 * NY,)), dma((8,)),
        dma((7,)), dma((7,)),
        dma((nz - 1,)), dma((nz - 1,)),
        dma((nz,)), dma((nz,)),
        dma((CHUNKS, nz)), dma((CHUNKS, nz)),
        dma((CHUNKS, nz // 2)), dma((CHUNKS,)),
        dma((2, CHUNKS)), dma((2, CHUNKS)),
        dma((2, CHUNKS)), dma((2, CHUNKS)),
        dma((2, CHUNKS)), dma((2, CHUNKS)),
        dma((MINE // 4,)), dma((MINE // 4,)),
        dma((2, CHUNKS)), dma((2, CHUNKS)),
        dma((2, CHUNKS)), dma((2, CHUNKS)),
        dma((2, CHUNKS)), dma((2, CHUNKS)),
    ]
    return pl.pallas_call(
        make_kernel(nx, nz),
        out_shape=(
            jax.ShapeDtypeStruct((T, H * D), BF16),
            jax.ShapeDtypeStruct((T, GROUPS * N), BF16),
            jax.ShapeDtypeStruct((T, GROUPS * N), BF16),
            jax.ShapeDtypeStruct((1, H), F32),
        ),
        in_specs=[pl.BlockSpec(memory_space=pltpu.VMEM)] * 9,
        out_specs=[pl.BlockSpec(memory_space=pltpu.VMEM)] * 4,
        scratch_shapes=scratch,
        compiler_params=pltpu.CompilerParams(vmem_limit_bytes=62 * 2**20, collective_id=0, has_side_effects=True),
        name="mixer_backward",
    )


def on_device(previous, saved_head_inputs, input_b, input_c, steps, decay_rate, skip_gain, segment_ids, advantage_mask):
    kernel = call(lax.axis_size("pipe"), lax.axis_size("seq_0"))
    gx, gb, gc, sk = kernel(
        previous[0],
        saved_head_inputs[0],
        input_b[0],
        input_c[0],
        steps[0],
        decay_rate,
        skip_gain,
        segment_ids,
        advantage_mask[None],
    )
    return gx[None], gb[None], gc[None], sk


def solution(mesh):
    finer = Mesh(
        mesh.devices.reshape(mesh.shape["pipe"], mesh.shape["seq"] // (2 * NY), NY, 2),
        ("pipe", "seq_0", "seq_1", "seq_2"),
    )
    return jax.shard_map(
        on_device,
        mesh=finer,
        in_specs=(
            P("pipe", SEQ, None),
            P("pipe", SEQ, None),
            P("pipe", SEQ, None),
            P("pipe", SEQ, None),
            P("pipe", SEQ, None),
            P("pipe", None),
            P("pipe", None),
            P("pipe", SEQ),
            P(SEQ),
        ),
        out_specs=(
            P("pipe", SEQ, None),
            P("pipe", SEQ, None),
            P("pipe", SEQ, None),
            P("pipe", None),
        ),
        check_vma=False,
    )
```

```python
import jax
import jax.numpy as jnp
from jax import lax
from jax.experimental import pallas as pl
from jax.experimental.pallas import tpu as pltpu
from jax.sharding import Mesh
from jax.sharding import PartitionSpec as P

SEQ = ("seq_0", "seq_1", "seq_2")
MESH = pl.DeviceIdType.MESH
F32 = jnp.float32
BF16 = jnp.bfloat16
NY = 4
T = 128
N = 128
H = 128
D = 64
GROUPS = 8
CHUNKS = 8
MINE = 2 * CHUNKS
ROWS = N // NY
QL = 256
QUARTERS = 32


def split(v, parts):
    out = []
    for _ in range(parts):
        piece = v.astype(BF16)
        out.append(piece)
        v = v - piece.astype(F32)
    return out


def dot(a, b):
    return lax.dot_general(a, b, (((1,), (0,)), ((), ())), preferred_element_type=F32)


def dot_nt(a, b):
    return lax.dot_general(a, b, (((1,), (1,)), ((), ())), preferred_element_type=F32)


def lanes_of(index, width):
    return pl.ds(pl.multiple_of(index * width, width), width)


def indicator(q, copies):
    row = lax.broadcasted_iota(jnp.int32, (H, QL), 0)
    col = lax.broadcasted_iota(jnp.int32, (H, QL), 1)
    one = jnp.where(row == 4 * q + lax.shift_right_logical(col, 6), 1.0, 0.0).astype(BF16)
    return jnp.concatenate([one] * copies, axis=0)


def make_kernel(nx, nz):
    width = (4, 2)
    count = (MINE // 4, CHUNKS)

    def kernel(
        prev_ref, x_hbm, b_hbm, c_hbm, steps_hbm, rate_ref, skip_ref, seg_ref, mask_ref,
        gx_out, gb_out, gc_out, sk_out,
        x_ref, b_ref, c_ref, steps_ref, lsem,
        grad, xo, gi, gxa, lexp, gca, gba, cum_s, cumt_s, bias_s, biast_s, eexp, lvs, bt, ct, wide_s, fz_s, fz_r, fzx,
        info_s, info_r, th_s, thx,
        st, sp, tt, t1, us, u2, zs, zr, az, ho, hi, vo, vi, eo, er, keep, epart, ex, tz_s,
        skp, sk_s, sk_r, skz_s, skz_r,
        gsend, grecv, isend, irecv, ssend, srecv, zsend, zrecv,
        fsend, frecv, asend, arecv, hsend, hrecv, dsend, drecv, t1send, t1recv, u2send, u2recv, csend, crecv, v2send, v2recv, e1send, e1recv, psend, precv,
    ):
        px = lax.axis_index("pipe")
        z = lax.axis_index("seq_0")
        y = lax.axis_index("seq_1")
        c = lax.axis_index("seq_2")
        d = 2 * y + c
        last_d = 2 * NY - 1

        def remote(src, dst, ssem, rsem, where):
            return pltpu.make_async_remote_copy(
                src_ref=src, dst_ref=dst, send_sem=ssem, recv_sem=rsem, device_id=where, device_id_type=MESH
            )

        def plane_peer(off):
            other = lax.rem(d + off, 2 * NY)
            return (px, z, lax.div(other, 2), lax.rem(other, 2))

        def z_peer(off):
            return (px, lax.rem(z + off, nz), y, c)

        loads = [
            pltpu.make_async_copy(src, dst, lsem.at[i])
            for i, (src, dst) in enumerate(
                ((steps_hbm, steps_ref), (b_hbm, b_ref), (c_hbm, c_ref), (x_hbm, x_ref), (prev_ref, grad))
            )
        ]
        for load in loads[:4]:
            load.start()

        @pl.when(px == nx - 1)
        def _():
            loads[4].start()

        barrier = pltpu.get_barrier_semaphore()

        def greet(where):
            pl.semaphore_signal(barrier, inc=1, device_id=where, device_id_type=MESH)

        for off in range(1, 2 * NY):
            greet(plane_peer(off))
        for off in range(1, nz):
            greet(z_peer(off))

        @pl.when(px < nx - 1)
        def _():
            greet((lax.rem(px + 1, nx), z, y, c))

        @pl.when(z > 0)
        def _():
            greet((px, lax.rem(z + nz - 1, nz), NY - 1, 1))

        from_next = (d == last_d) & (z < nz - 1)
        callers = 2 * NY - 1 + nz - 1 + jnp.where(px > 0, 1, 0) + jnp.where(from_next, 2 * NY, 0)
        pl.semaphore_wait(barrier, callers)

        def grad_copy(k):
            part = lanes_of(k, 4 * QL)
            return remote(
                prev_ref.at[:, part], grad.at[:, part], gsend.at[k], grecv.at[k], (lax.rem(px + nx - 1, nx), z, y, c)
            )

        @pl.when(px > 0)
        def _():
            def body(k, carry):
                grad_copy(k).start()
                return carry

            lax.fori_loop(0, CHUNKS, body, 0)

        row = lax.broadcasted_iota(jnp.int32, (T, T), 0)
        col = lax.broadcasted_iota(jnp.int32, (T, T), 1)
        loads[0].wait()
        cum = -(steps_ref[...] * rate_ref[...])
        for shift in (1, 2, 4, 8, 16, 32, 64):
            cum = cum + jnp.where(row >= shift, pltpu.roll(cum, shift, 0), 0.0)
        cum_s[...] = cum
        cumt_s[...] = cum.T
        last = cum[T - 1 : T, :]
        segrow = jnp.broadcast_to(seg_ref[...].astype(F32), (T, T))
        segcol = segrow.T
        seglast = segcol[T - 1 : T, :]
        info_s[0:1, :] = last
        info_s[1:2, :] = seglast
        info_s[2:8, :] = jnp.zeros((6, H), F32)
        info_r[d] = info_s[...]

        def info_copy(off):
            return remote(info_s, info_r.at[d], isend.at[off - 1], irecv.at[off - 1], plane_peer(off))

        def info_next(other):
            return remote(
                info_s, info_r.at[2 * NY], isend.at[7 + other], irecv.at[7], (px, lax.rem(z + 1, nz), other // 2, other % 2)
            )

        for off in range(1, 2 * NY):
            info_copy(off).start()

        @pl.when((d == last_d) & (z < nz - 1))
        def _():
            for other in range(2 * NY):
                info_next(other).start()

        @pl.when(z == 0)
        def _():
            info_r[2 * NY] = jnp.full((8, H), -1.0, F32)

        linked = segcol == segrow
        bias_s[...] = jnp.where(linked & (row >= col), 0.0, -1e30)
        biast_s[...] = jnp.where(linked & (col >= row), 0.0, -1e30)
        leave = jnp.exp(last - cum) * jnp.where(segcol == seglast, 1.0, 0.0)
        lvs[...] = jnp.concatenate(split(leave, 2), axis=1)
        kept = jnp.broadcast_to(mask_ref[...].astype(F32), (T, T)).T
        wide_s[...] = jnp.concatenate([kept, kept], axis=1)

        for load in loads[1:4]:
            load.wait()

        @pl.when(px == nx - 1)
        def _():
            loads[4].wait()

        for g in range(GROUPS):
            part = slice(N * g, N * g + N)
            bt[g] = b_ref[:, part].astype(F32).T.astype(BF16)
            ct[g] = c_ref[:, part].astype(F32).T.astype(BF16)

        pair = lax.div(y, 2)
        low_y = lax.rem(y, 2)
        half_of = jnp.where(low_y == pair, 0, 1)
        in_pair = (px, z, 2 * pair + 1 - low_y, c)
        over_pairs = (px, z, NY - 1 - y, c)

        mine = c
        theirs = 1 - c

        def some(ref, w, k):
            return ref.at[w, pl.ds(width[w] * k, width[w])]

        def partner_copy(w, k):
            n = width[w]
            return remote(
                st.at[w, theirs, pl.ds(n * k, n)], some(sp, w, k), dsend.at[w, k], drecv.at[w, k], (px, z, y, 1 - c)
            )

        def quarter(m, side):
            return 4 * lax.div(m, 2) + 2 * side + lax.rem(m, 2)

        def states(w, k, side):
            for i in range(width[w]):
                m = width[w] * k + i
                q = quarter(m, side)
                g = lax.div(m, 2)
                part = lanes_of(q, QL)
                if w == 0:
                    factor = dot(lvs[...], indicator(q, 2))
                    lexp[q] = factor
                    moved = (factor * x_ref[:, part].astype(F32)).astype(BF16)
                    xo[q] = moved
                    st[w, side, m] = dot(bt[g], moved).astype(BF16)
                else:
                    gr = grad[:, part].astype(F32)
                    moved = (eexp[q] * gr).astype(BF16)
                    gi[q] = moved
                    st[w, side, m] = dot(ct[g], moved).astype(BF16)
                    skp[q] = jnp.sum(gr * x_ref[:, part].astype(F32), axis=0, keepdims=True)

        def t_copy(w, k):
            m = pl.ds(width[w] * k, width[w])
            return remote(tt.at[w, m, 1 - half_of], t1.at[w, m], t1send.at[w, k], t1recv.at[w, k], in_pair)

        def u_copy(w, k):
            m = pl.ds(width[w] * k, width[w])
            return remote(us.at[w, m, 1 - pair], u2.at[w, m], u2send.at[w, k], u2recv.at[w, k], over_pairs)

        def v_copy(w, k):
            m = pl.ds(width[w] * k, width[w])
            return remote(vo.at[w, m], vi.at[w, m, pair], v2send.at[w, k], v2recv.at[w, k], over_pairs)

        def e_copy(w, k):
            m = pl.ds(width[w] * k, width[w])
            return remote(eo.at[w, m], er.at[w, m, half_of], e1send.at[w, k], e1recv.at[w, k], in_pair)

        def chip_decay(q, chip):
            return thx[q, pl.ds(2 * chip, 1), :] * thx[q, pl.ds(2 * chip + 1, 1), :]

        def pair_decay(q, which):
            return chip_decay(q, 2 * which) * chip_decay(q, 2 * which + 1)

        def chip_state(w, k):
            up, down = (0, 1) if w == 0 else (1, 0)
            partner_copy(w, k).wait_recv()
            for i in range(width[w]):
                m = width[w] * k + i
                own = st[w, mine, m].astype(F32)
                other = sp[w, m].astype(F32)
                first = jnp.where(c == up, own, other)
                second = jnp.where(c == up, other, own)
                decay = thx[quarter(m, mine), pl.ds(2 * y + down, 1), :]
                tt[w, m] = (decay * first + second).astype(BF16).reshape(2, 2 * ROWS, QL)
            t_copy(w, k).start()

        def pair_first(w, m):
            own = tt[w, m, half_of].astype(F32)
            other = t1[w, m].astype(F32)
            return jnp.where(low_y == w, own, other), jnp.where(low_y == w, other, own)

        def pair_step(w, k):
            t_copy(w, k).wait_recv()
            for i in range(width[w]):
                m = width[w] * k + i
                first, second = pair_first(w, m)
                decay = chip_decay(quarter(m, mine), 2 * pair + 1 - w)
                us[w, m] = (decay * first + second).astype(BF16).reshape(2, ROWS, QL)
            u_copy(w, k).start()

        def plane_first(w, m):
            own = us[w, m, pair].astype(F32)
            other = u2[w, m].astype(F32)
            return jnp.where(pair == w, own, other), jnp.where(pair == w, other, own)

        def chain_copy(k):
            m = pl.ds(width[0] * k, width[0])
            return remote(zs.at[m], zr.at[m], csend.at[k], crecv.at[k], z_peer(1))

        def across(k, other):
            m = pl.ds(width[1] * k, width[1])
            return remote(az.at[z, m], az.at[z, m], asend.at[k, other], arecv.at[k, z], (px, other, y, c))

        half = nz // 2
        start = half * lax.div(z, half)

        def down(k, other):
            m = pl.ds(width[1] * k, width[1])
            return remote(ho.at[m], hi.at[m], hsend.at[k, other], hrecv.at[k], (px, other, y, c))

        def arrived(k, source):
            m = pl.ds(width[1] * k, width[1])
            return remote(az.at[source, m], az.at[source, m], asend.at[k, source], arecv.at[k, source], (px, source, y, c))

        def plane_total(w, m):
            q = quarter(m, mine)
            first, second = plane_first(w, m)
            decay = pair_decay(q, 1 - w)
            return decay * first + second, decay * pair_decay(q, w)

        def spread_out(w, k, values):
            for i, value in enumerate(values):
                m = width[w] * k + i
                after = pair_decay(quarter(m, mine), w) * value + plane_first(w, m)[0]
                vi[w, m, pair] = jnp.where(pair == w, value, after).astype(BF16)
                vo[w, m] = jnp.where(pair == w, after, value).astype(BF16)
            v_copy(w, k).start()

        def pair_out(w, k):
            v_copy(w, k).wait_recv()
            for i in range(width[w]):
                m = width[w] * k + i
                value = vi[w, m].reshape(2 * ROWS, QL).astype(F32)
                after = chip_decay(quarter(m, mine), 2 * pair + w) * value + pair_first(w, m)[0]
                er[w, m, half_of] = jnp.where(low_y == w, value, after).astype(BF16)
                eo[w, m] = jnp.where(low_y == w, after, value).astype(BF16)
            e_copy(w, k).start()

        def chain(k):
            u_copy(0, k).wait_recv()
            held = []
            for i in range(width[0]):
                m = width[0] * k + i
                total, factor = plane_total(0, m)
                tz_s[i] = total
                held.append((m, factor))

            @pl.when(z == 0)
            def _():
                for m, _factor in held:
                    zr[m] = jnp.zeros((ROWS, QL), BF16)

            @pl.when(z > 0)
            def _():
                chain_copy(k).wait_recv()

            @pl.when(z < nz - 1)
            def _():
                for i, (m, factor) in enumerate(held):
                    zs[m] = (factor * zr[m].astype(F32) + tz_s[i]).astype(BF16)
                chain_copy(k).start()

            spread_out(0, k, [zr[m].astype(F32) for m, _factor in held])

        def plane_send(k):
            u_copy(1, k).wait_recv()
            for i in range(width[1]):
                m = width[1] * k + i
                az[z, m] = plane_total(1, m)[0].astype(BF16)

            def body(other, carry):
                across(k, other).start()
                return carry

            lax.fori_loop(start, z, body, 0)

        def plane_back(k):
            @pl.when(z >= half)
            def _():
                for i in range(width[1]):
                    tz_s[i] = jnp.zeros((ROWS, QL), F32)

            @pl.when(z < half)
            def _():
                down(k, half).wait_recv()
                for i in range(width[1]):
                    tz_s[i] = hi[width[1] * k + i].astype(F32)

            def body(t, carry):
                source = start + half - 1 - t
                arrived(k, source).wait_recv()
                for i in range(width[1]):
                    m = width[1] * k + i
                    factor = fzx[quarter(m, mine), pl.ds(source, 1), :]
                    tz_s[i] = factor * tz_s[i] + az[source, m].astype(F32)
                return carry

            lax.fori_loop(0, start + half - 1 - z, body, 0)

            @pl.when(z == half)
            def _():
                for i in range(width[1]):
                    m = width[1] * k + i
                    total, factor = plane_total(1, m)
                    ho[m] = (factor * tz_s[i] + total).astype(BF16)
                for other in range(half):
                    down(k, other).start()

            spread_out(1, k, [tz_s[i] for i in range(width[1])])

        def back_copy(w, k):
            return remote(some(epart, w, k), some(ex, w, k), psend.at[w, k], precv.at[w, k], (px, z, y, 1 - c))

        def hand_back(w, k):
            up = 0 if w == 0 else 1
            e_copy(w, k).wait_recv()
            for i in range(width[w]):
                m = width[w] * k + i
                here = er[w, m].reshape(N, QL).astype(F32)
                first = jnp.where(c == up, st[w, mine, m].astype(F32), sp[w, m].astype(F32))
                decay = thx[quarter(m, mine), pl.ds(2 * y + up, 1), :]
                after = decay * here + first
                keep[w, m] = jnp.where(c == up, here, after).astype(BF16)
                epart[w, m] = jnp.where(c == up, after, here).astype(BF16)
            back_copy(w, k).start()

        def finish_c(k):
            back_copy(0, k).wait_recv()
            for j in range(2):
                g = 2 * k + j
                acc = gca[g]
                for i in range(2):
                    m = 2 * g + i
                    acc = acc + dot_nt(gi[quarter(m, mine)], keep[0, m]) + dot_nt(gi[quarter(m, theirs)], ex[0, m])
                gc_out[:, lanes_of(g, N)] = acc.astype(BF16)

        def finish_b(g):
            back_copy(1, g).wait_recv()
            bg = b_ref[:, lanes_of(g, N)]
            acc = gba[g]
            for side, source in ((mine, keep), (theirs, ex)):
                for i in range(2):
                    m = 2 * g + i
                    q = quarter(m, side)
                    later = source[1, m]
                    acc = acc + dot_nt(xo[q], later)
                    gx_out[:, lanes_of(q, QL)] = (gxa[q] + lexp[q] * dot(bg, later)).astype(BF16)
            gb_out[:, lanes_of(g, N)] = acc.astype(BF16)

        def fwd_states(k, carry):
            states(0, k, theirs)
            partner_copy(0, k).start()
            states(0, k, mine)
            return carry

        lax.fori_loop(0, count[0], fwd_states, 0)

        for off in range(1, 2 * NY):
            info_copy(off).wait_recv()

        @pl.when(z > 0)
        def _():
            remote(info_s, info_r.at[2 * NY], isend.at[7], irecv.at[7], z_peer(nz - 1)).wait_recv()

        th_s[...] = jnp.zeros((16, H), F32)
        for i in range(2 * NY):
            before = info_r[2 * NY if i == 0 else i - 1, 1:2, :]
            th_s[i : i + 1, :] = jnp.exp(info_r[i, 0:1, :]) * jnp.where(info_r[i, 1:2, :] == before, 1.0, 0.0)
        th_s[8:9, :] = skip_ref[...]
        enter_from = info_r[lax.rem(d + 2 * NY, 2 * NY + 1), 1:2, :]
        segc = jnp.broadcast_to(seg_ref[...].astype(F32), (T, T)).T
        enter = jnp.exp(cum_s[...]) * jnp.where(segc == enter_from, 1.0, 0.0)
        lvs[...] = jnp.concatenate(split(enter, 2), axis=1)
        whole = th_s[0:1, :]
        for i in range(1, 2 * NY):
            whole = whole * th_s[i : i + 1, :]
        fz_s[...] = jnp.broadcast_to(whole, (8, H))
        fz_r[z] = fz_s[...]

        def f_copy(other):
            return remote(fz_s, fz_r.at[z], fsend.at[other], frecv.at[z], (px, other, y, c))

        def f_arrived(source):
            return remote(fz_s, fz_r.at[source], fsend.at[source], frecv.at[source], (px, source, y, c))

        def f_start(other, carry):
            f_copy(other).start()
            return carry

        lax.fori_loop(0, z, f_start, 0)

        def table(k, carry):
            rows = jnp.concatenate(split(th_s[...], 3), axis=1)
            for i in range(4):
                thx[4 * k + i] = dot(rows, indicator(4 * k + i, 3))
            return carry

        lax.fori_loop(0, QUARTERS // 4, table, 0)

        def fwd_chip(k, carry):
            chip_state(0, k)
            return carry

        lax.fori_loop(0, count[0], fwd_chip, 0)

        def enter_wide(k, carry):
            for i in range(4):
                eexp[4 * k + i] = dot(lvs[...], indicator(4 * k + i, 2))
            return carry

        enter_wide(0, 0)

        def f_wait(t, carry):
            f_arrived(nz - 1 - t).wait_recv()
            return carry

        def plane_table():
            lax.fori_loop(0, nz - 1 - z, f_wait, 0)
            everything = jnp.concatenate(
                [jnp.where(i > z, fz_r[i, 0:1, :], 0.0) for i in range(nz)], axis=0
            )
            th_s[0:nz, :] = everything

            def body(k, carry):
                rows = jnp.concatenate(split(th_s[...], 3), axis=1)
                for i in range(4):
                    fzx[4 * k + i] = dot(rows, indicator(4 * k + i, 3))
                return carry

            lax.fori_loop(0, QUARTERS // 4, body, 0)

        def within(g):
            bg = b_ref[:, lanes_of(g, N)]
            cg = c_ref[:, lanes_of(g, N)]
            cross = dot_nt(bg, cg)
            cols = pltpu.roll(cum_s[...], lax.rem(H - 16 * g, H), 1)
            low = lax.broadcasted_iota(jnp.int32, (T, T), 1) < D
            total = jnp.zeros((T, T), F32)
            for j in range(8):
                part = pl.ds(pl.multiple_of(1024 * g + 128 * j, 128), 128)
                gf = grad[:, part].astype(F32)
                xp = x_ref[:, part]
                both = jnp.concatenate(
                    [jnp.where(low, gf, 0.0).astype(BF16), jnp.where(low, 0.0, gf).astype(BF16)], axis=0
                )
                prod = dot_nt(both, xp)
                pieces = []
                for i in range(2):
                    j2 = 2 * j + i
                    spread = cols[:, j2 : j2 + 1] - cumt_s[pl.ds(16 * g + j2, 1), :]
                    total = total + jnp.exp(spread + bias_s[...]) * prod[T * i : T * i + T, :]
                    pieces.append((jnp.exp(biast_s[...] - spread) * cross).astype(BF16))
                out = dot(jnp.concatenate(pieces, axis=1), both)
                half = slice(128 * (j % 2), 128 * (j % 2) + 128)
                q = 4 * g + j // 2
                gxa[q, :, half] = out + thx[q, 8:9, half] * gf
            gca[g] = dot(total.astype(BF16), bg)
            gba[g] = dot(total.T.astype(BF16), cg)

        def sk_copy(off):
            return remote(sk_s, sk_r.at[d], ssend.at[off - 1], srecv.at[off - 1], plane_peer(off))

        def skz_copy(off):
            return remote(skz_s, skz_r.at[z], zsend.at[off - 1], zrecv.at[off - 1], z_peer(off))

        def sk_plane():
            row_q = lax.broadcasted_iota(jnp.int32, (QL, 128), 0)
            col_q = lax.broadcasted_iota(jnp.int32, (QL, 128), 1)
            pick = jnp.where(lax.shift_right_logical(row_q, 6) == (col_q & 3), 1.0, 0.0).astype(BF16)
            sums = jnp.reshape(skp[...], (QUARTERS, QL))
            heads = sum(dot(piece, pick) for piece in split(sums, 3))
            own_row = lax.broadcasted_iota(jnp.int32, (QUARTERS, 128), 0)
            own_col = lax.broadcasted_iota(jnp.int32, (QUARTERS, 128), 1)
            heads = jnp.where(lax.shift_right_logical(own_col, 2) == own_row, heads, 0.0)
            sk_s[...] = jnp.broadcast_to(jnp.sum(heads, axis=0, keepdims=True), (8, 128))
            sk_r[d] = sk_s[...]
            for off in range(1, 2 * NY):
                sk_copy(off).start()

        def sk_along():
            for off in range(1, 2 * NY):
                sk_copy(off).wait_recv()
            acc = sk_r[0]
            for i in range(1, 2 * NY):
                acc = acc + sk_r[i]
            skz_s[...] = acc
            skz_r[z] = acc
            for off in range(1, nz):
                skz_copy(off).start()

        def each(n, step):
            def body(k, carry):
                step(k)
                return carry

            lax.fori_loop(0, n, body, 0)

        chain_at = 2 + lax.div(z * 5 + 3, nz - 1)
        back_at = jnp.where(z < half, 4, 3)

        def main(k, carry):
            def at(lag, n, step):
                @pl.when((k >= lag) & (k < lag + n))
                def _():
                    step(k - lag)

            def begin(k):
                @pl.when(px == nx - 1)
                def _():
                    for i in range(4):
                        part = lanes_of(4 * k + i, QL)
                        grad[:, part] = (grad[:, part].astype(F32) * wide_s[...]).astype(BF16)

                @pl.when(px < nx - 1)
                def _():
                    grad_copy(k).wait_recv()

                states(1, k, theirs)
                partner_copy(1, k).start()
                states(1, k, mine)

                @pl.when(k < CHUNKS - 1)
                def _():
                    enter_wide(k + 1, 0)

                chip_state(1, k)
                within(k)

            at(0, CHUNKS, begin)

            @pl.when(k == 1)
            def _():
                plane_table()

            @pl.when(k == CHUNKS)
            def _():
                sk_plane()

            def at_pairing_end(lag, n, step):
                @pl.when((k >= lag) & (k < lag + n - 1))
                def _():
                    step(k - lag)

                @pl.when(k == lag + n - 2)
                def _():
                    step(k - lag + 1)

            def two(step):
                def both(i):
                    step(2 * i)
                    step(2 * i + 1)

                return both

            at_pairing_end(1, count[1], lambda i: pair_step(1, i))
            at_pairing_end(2, count[1], plane_send)
            at_pairing_end(back_at, count[1], plane_back)
            at_pairing_end(back_at + 1, count[1], lambda i: pair_out(1, i))
            at_pairing_end(back_at + 2, count[1], lambda i: hand_back(1, i))

            @pl.when(k == CHUNKS + 2)
            def _():
                sk_along()

            at_pairing_end(back_at + 3, count[1], finish_b)
            at(1, count[0] // 2, two(lambda i: pair_step(0, i)))
            at(chain_at, count[0] // 2, two(chain))
            at(chain_at + 1, count[0], lambda i: pair_out(0, i))
            at(chain_at + 2, count[0], lambda i: hand_back(0, i))
            at(chain_at + 3, count[0], finish_c)
            return carry

        lax.fori_loop(0, CHUNKS + 6, main, 0)

        for off in range(1, nz):
            skz_copy(off).wait_recv()
        acc = skz_r[0]
        for i in range(1, nz):
            acc = acc + skz_r[i]
        sk_out[...] = acc[0:1, :]

        @pl.when(px > 0)
        def _():
            def body(k, carry):
                grad_copy(k).wait_send()
                return carry

            lax.fori_loop(0, CHUNKS, body, 0)

        for off in range(1, 2 * NY):
            info_copy(off).wait_send()
            sk_copy(off).wait_send()

        @pl.when((d == last_d) & (z < nz - 1))
        def _():
            for other in range(2 * NY):
                info_next(other).wait_send()

        for off in range(1, nz):
            skz_copy(off).wait_send()

        for w in range(2):

            def drain(k, w=w):
                partner_copy(w, k).wait_send()
                back_copy(w, k).wait_send()
                t_copy(w, k).wait_send()
                u_copy(w, k).wait_send()
                v_copy(w, k).wait_send()
                e_copy(w, k).wait_send()
                if w == 0:

                    @pl.when(z < nz - 1)
                    def _():
                        chain_copy(k).wait_send()
                else:

                    def let_go(other, carry, k=k):
                        across(k, other).wait_send()
                        return carry

                    lax.fori_loop(start, z, let_go, 0)

                    @pl.when(z == half)
                    def _():
                        for other in range(half):
                            down(k, other).wait_send()


            each(count[w], drain)
        each(z, lambda other: f_copy(other).wait_send())

    return kernel


def call(nx, nz):
    vm = pltpu.VMEM
    dma = pltpu.SemaphoreType.DMA
    scratch = [
        vm((T, H * D), BF16),
        vm((T, GROUPS * N), BF16),
        vm((T, GROUPS * N), BF16),
        vm((T, H), F32),
        dma((5,)),
        vm((T, H * D), BF16),
        vm((QUARTERS, T, QL), BF16),
        vm((QUARTERS, T, QL), BF16),
        vm((QUARTERS, T, QL), F32),
        vm((QUARTERS, T, QL), F32),
        vm((GROUPS, T, N), F32),
        vm((GROUPS, T, N), F32),
        vm((T, H), F32),
        vm((H, T), F32),
        vm((T, T), F32),
        vm((T, T), F32),
        vm((QUARTERS, T, QL), F32),
        vm((T, 2 * H), BF16),
        vm((GROUPS, N, T), BF16),
        vm((GROUPS, N, T), BF16),
        vm((T, QL), F32),
        vm((8, H), F32),
        vm((nz, 8, H), F32),
        vm((QUARTERS, 16, QL), F32),
        vm((8, H), F32),
        vm((2 * NY + 1, 8, H), F32),
        vm((16, H), F32),
        vm((QUARTERS, 16, QL), F32),
        vm((2, 2, MINE, N, QL), BF16),
        vm((2, MINE, N, QL), BF16),
        vm((2, MINE, 2, 2 * ROWS, QL), BF16),
        vm((2, MINE, 2 * ROWS, QL), BF16),
        vm((2, MINE, 2, ROWS, QL), BF16),
        vm((2, MINE, ROWS, QL), BF16),
        vm((MINE, ROWS, QL), BF16),
        vm((MINE, ROWS, QL), BF16),
        vm((nz, MINE, ROWS, QL), BF16),
        vm((MINE, ROWS, QL), BF16),
        vm((MINE, ROWS, QL), BF16),
        vm((2, MINE, ROWS, QL), BF16),
        vm((2, MINE, 2, ROWS, QL), BF16),
        vm((2, MINE, 2 * ROWS, QL), BF16),
        vm((2, MINE, 2, 2 * ROWS, QL), BF16),
        vm((2, MINE, N, QL), BF16),
        vm((2, MINE, N, QL), BF16),
        vm((2, MINE, N, QL), BF16),
        vm((4, ROWS, QL), F32),
        vm((QUARTERS, 1, QL), F32),
        vm((8, 128), F32),
        vm((2 * NY, 8, 128), F32),
        vm((8, 128), F32),
        vm((nz, 8, 128), F32),
        dma((CHUNKS,)), dma((CHUNKS,)),
        dma((7 + 2 * NY,)), dma((8,)),
        dma((7,)), dma((7,)),
        dma((nz - 1,)), dma((nz - 1,)),
        dma((nz,)), dma((nz,)),
        dma((CHUNKS, nz)), dma((CHUNKS, nz)),
        dma((CHUNKS, nz // 2)), dma((CHUNKS,)),
        dma((2, CHUNKS)), dma((2, CHUNKS)),
        dma((2, CHUNKS)), dma((2, CHUNKS)),
        dma((2, CHUNKS)), dma((2, CHUNKS)),
        dma((MINE // 4,)), dma((MINE // 4,)),
        dma((2, CHUNKS)), dma((2, CHUNKS)),
        dma((2, CHUNKS)), dma((2, CHUNKS)),
        dma((2, CHUNKS)), dma((2, CHUNKS)),
    ]
    return pl.pallas_call(
        make_kernel(nx, nz),
        out_shape=(
            vm((T, H * D), BF16),
            vm((T, GROUPS * N), BF16),
            vm((T, GROUPS * N), BF16),
            vm((1, H), F32),
        ),
        in_specs=[pl.BlockSpec(memory_space=pl.ANY)] * 5 + [pl.BlockSpec(memory_space=pltpu.VMEM)] * 4,
        out_specs=[pl.BlockSpec(memory_space=pltpu.VMEM)] * 4,
        scratch_shapes=scratch,
        compiler_params=pltpu.CompilerParams(vmem_limit_bytes=56 * 2**20, collective_id=0, has_side_effects=True),
        name="mixer_backward",
    )


def deliver(*results):
    def kernel(*refs):
        n = len(results)
        sem = refs[2 * n]
        copies = [pltpu.make_async_copy(refs[i], refs[n + i], sem.at[i]) for i in range(n)]
        for copy in copies:
            copy.start()
        for copy in copies:
            copy.wait()

    return pl.pallas_call(
        kernel,
        out_shape=tuple(jax.ShapeDtypeStruct(v.shape, v.dtype) for v in results),
        in_specs=[pl.BlockSpec(memory_space=pltpu.VMEM)] * len(results),
        out_specs=[pl.BlockSpec(memory_space=pl.ANY)] * len(results),
        scratch_shapes=[pltpu.SemaphoreType.DMA((len(results),))],
        compiler_params=pltpu.CompilerParams(vmem_limit_bytes=2**20),
        name="deliver",
    )(*results)


def on_device(previous, saved_head_inputs, input_b, input_c, steps, decay_rate, skip_gain, segment_ids, advantage_mask):
    kernel = call(lax.axis_size("pipe"), lax.axis_size("seq_0"))
    gx, gb, gc, sk = kernel(
        previous[0],
        saved_head_inputs[0],
        input_b[0],
        input_c[0],
        steps[0],
        decay_rate,
        skip_gain,
        segment_ids,
        advantage_mask[None],
    )
    gx, gb, gc, sk = deliver(gx, gb, gc, sk)
    return gx[None], gb[None], gc[None], sk


def solution(mesh):
    finer = Mesh(
        mesh.devices.reshape(mesh.shape["pipe"], mesh.shape["seq"] // (2 * NY), NY, 2),
        ("pipe", "seq_0", "seq_1", "seq_2"),
    )
    return jax.shard_map(
        on_device,
        mesh=finer,
        in_specs=(
            P("pipe", SEQ, None),
            P("pipe", SEQ, None),
            P("pipe", SEQ, None),
            P("pipe", SEQ, None),
            P("pipe", SEQ, None),
            P("pipe", None),
            P("pipe", None),
            P("pipe", SEQ),
            P(SEQ),
        ),
        out_specs=(
            P("pipe", SEQ, None),
            P("pipe", SEQ, None),
            P("pipe", SEQ, None),
            P("pipe", None),
        ),
        check_vma=False,
    )
```

```python
import jax
import jax.numpy as jnp
from jax import lax
from jax.experimental import pallas as pl
from jax.experimental.pallas import tpu as pltpu
from jax.sharding import Mesh
from jax.sharding import PartitionSpec as P

SEQ = ("seq_0", "seq_1", "seq_2")
MESH = pl.DeviceIdType.MESH
F32 = jnp.float32
BF16 = jnp.bfloat16
NY = 4
T = 128
N = 128
H = 128
D = 64
GROUPS = 8
CHUNKS = 8
MINE = 2 * CHUNKS
ROWS = N // NY
QL = 256
QUARTERS = 32


def split(v, parts):
    out = []
    for _ in range(parts):
        piece = v.astype(BF16)
        out.append(piece)
        v = v - piece.astype(F32)
    return out


def dot(a, b):
    return lax.dot_general(a, b, (((1,), (0,)), ((), ())), preferred_element_type=F32)


def dot_nt(a, b):
    return lax.dot_general(a, b, (((1,), (1,)), ((), ())), preferred_element_type=F32)


def lanes_of(index, width):
    return pl.ds(pl.multiple_of(index * width, width), width)


def indicator(q, copies):
    row = lax.broadcasted_iota(jnp.int32, (H, QL), 0)
    col = lax.broadcasted_iota(jnp.int32, (H, QL), 1)
    one = jnp.where(row == 4 * q + lax.shift_right_logical(col, 6), 1.0, 0.0).astype(BF16)
    return jnp.concatenate([one] * copies, axis=0)


def make_kernel(nx, nz):
    width = (4, 2)
    count = (MINE // 4, CHUNKS)

    def kernel(
        prev_ref, x_hbm, b_hbm, c_hbm, steps_hbm, rate_ref, skip_ref, seg_ref, mask_ref,
        gx_out, gb_out, gc_out, sk_out,
        x_ref, b_ref, c_ref, steps_ref, lsem,
        grad, xo, gi, gxa, lexp, gca, gba, cum_s, cumt_s, bias_s, biast_s, eexp, lvs, bt, ct, wide_s, fz_s, fz_r, fzx,
        info_s, info_r, th_s, thx,
        st, sp, tt, t1, us, u2, zs, zr, az, ho, hi, vo, vi, eo, er, keep, epart, ex, tz_s,
        skp, sk_s, sk_r, skz_s, skz_r,
        gsend, grecv, isend, irecv, ssend, srecv, zsend, zrecv,
        fsend, frecv, asend, arecv, hsend, hrecv, dsend, drecv, t1send, t1recv, u2send, u2recv, csend, crecv, v2send, v2recv, e1send, e1recv, psend, precv,
    ):
        px = lax.axis_index("pipe")
        z = lax.axis_index("seq_0")
        y = lax.axis_index("seq_1")
        c = lax.axis_index("seq_2")
        d = 2 * y + c
        last_d = 2 * NY - 1
        half = nz // 2
        start = half * lax.div(z, half)
        to_top = (z >= half) & (z < nz - 1)

        def remote(src, dst, ssem, rsem, where):
            return pltpu.make_async_remote_copy(
                src_ref=src, dst_ref=dst, send_sem=ssem, recv_sem=rsem, device_id=where, device_id_type=MESH
            )

        def plane_peer(off):
            other = lax.rem(d + off, 2 * NY)
            return (px, z, lax.div(other, 2), lax.rem(other, 2))

        def z_peer(off):
            return (px, lax.rem(z + off, nz), y, c)

        loads = [
            pltpu.make_async_copy(src, dst, lsem.at[i])
            for i, (src, dst) in enumerate(
                ((steps_hbm, steps_ref), (b_hbm, b_ref), (c_hbm, c_ref), (x_hbm, x_ref), (prev_ref, grad))
            )
        ]
        for load in loads[:4]:
            load.start()

        @pl.when(px == nx - 1)
        def _():
            loads[4].start()

        barrier = pltpu.get_barrier_semaphore()

        def greet(where):
            pl.semaphore_signal(barrier, inc=1, device_id=where, device_id_type=MESH)

        for off in range(1, 2 * NY):
            greet(plane_peer(off))
        for off in range(1, nz):
            greet(z_peer(off))

        @pl.when(px < nx - 1)
        def _():
            greet((lax.rem(px + 1, nx), z, y, c))

        @pl.when(z > 0)
        def _():
            greet((px, lax.rem(z + nz - 1, nz), NY - 1, 1))

        from_next = (d == last_d) & (z < nz - 1)
        callers = 2 * NY - 1 + nz - 1 + jnp.where(px > 0, 1, 0) + jnp.where(from_next, 2 * NY, 0)
        pl.semaphore_wait(barrier, callers)

        def grad_copy(k):
            part = lanes_of(k, 4 * QL)
            return remote(
                prev_ref.at[:, part], grad.at[:, part], gsend.at[k], grecv.at[k], (lax.rem(px + nx - 1, nx), z, y, c)
            )

        @pl.when(px > 0)
        def _():
            def body(k, carry):
                grad_copy(k).start()
                return carry

            lax.fori_loop(0, CHUNKS, body, 0)

        row = lax.broadcasted_iota(jnp.int32, (T, T), 0)
        col = lax.broadcasted_iota(jnp.int32, (T, T), 1)
        loads[0].wait()
        cum = -(steps_ref[...] * rate_ref[...])
        for shift in (1, 2, 4, 8, 16, 32, 64):
            cum = cum + jnp.where(row >= shift, pltpu.roll(cum, shift, 0), 0.0)
        cum_s[...] = cum
        cumt_s[...] = cum.T
        last = cum[T - 1 : T, :]
        segrow = jnp.broadcast_to(seg_ref[...].astype(F32), (T, T))
        segcol = segrow.T
        seglast = segcol[T - 1 : T, :]
        info_s[0:1, :] = last
        info_s[1:2, :] = seglast
        info_s[2:8, :] = jnp.zeros((6, H), F32)
        info_r[d] = info_s[...]

        def info_copy(off):
            return remote(info_s, info_r.at[d], isend.at[off - 1], irecv.at[off - 1], plane_peer(off))

        def info_next(other):
            return remote(
                info_s, info_r.at[2 * NY], isend.at[7 + other], irecv.at[7], (px, lax.rem(z + 1, nz), other // 2, other % 2)
            )

        for off in range(1, 2 * NY):
            info_copy(off).start()

        @pl.when((d == last_d) & (z < nz - 1))
        def _():
            for other in range(2 * NY):
                info_next(other).start()

        @pl.when(z == 0)
        def _():
            info_r[2 * NY] = jnp.full((8, H), -1.0, F32)

        linked = segcol == segrow
        bias_s[...] = jnp.where(linked & (row >= col), 0.0, -1e30)
        biast_s[...] = jnp.where(linked & (col >= row), 0.0, -1e30)
        leave = jnp.exp(last - cum) * jnp.where(segcol == seglast, 1.0, 0.0)
        lvs[...] = jnp.concatenate(split(leave, 2), axis=1)
        kept = jnp.broadcast_to(mask_ref[...].astype(F32), (T, T)).T
        wide_s[...] = jnp.concatenate([kept, kept], axis=1)

        for load in loads[1:4]:
            load.wait()

        @pl.when(px == nx - 1)
        def _():
            loads[4].wait()

        for g in range(GROUPS):
            part = slice(N * g, N * g + N)
            bt[g] = b_ref[:, part].astype(F32).T.astype(BF16)
            ct[g] = c_ref[:, part].astype(F32).T.astype(BF16)

        pair = lax.div(y, 2)
        low_y = lax.rem(y, 2)
        half_of = jnp.where(low_y == pair, 0, 1)
        in_pair = (px, z, 2 * pair + 1 - low_y, c)
        over_pairs = (px, z, NY - 1 - y, c)

        mine = c
        theirs = 1 - c

        def some(ref, w, k):
            return ref.at[w, pl.ds(width[w] * k, width[w])]

        def partner_copy(w, k):
            n = width[w]
            return remote(
                st.at[w, theirs, pl.ds(n * k, n)], some(sp, w, k), dsend.at[w, k], drecv.at[w, k], (px, z, y, 1 - c)
            )

        def quarter(m, side):
            return 4 * lax.div(m, 2) + 2 * side + lax.rem(m, 2)

        def states(w, k, side):
            for i in range(width[w]):
                m = width[w] * k + i
                q = quarter(m, side)
                g = lax.div(m, 2)
                part = lanes_of(q, QL)
                if w == 0:
                    factor = dot(lvs[...], indicator(q, 2))
                    lexp[q] = factor
                    moved = (factor * x_ref[:, part].astype(F32)).astype(BF16)
                    xo[q] = moved
                    st[w, side, m] = dot(bt[g], moved).astype(BF16)
                else:
                    gr = grad[:, part].astype(F32)
                    moved = (eexp[q] * gr).astype(BF16)
                    gi[q] = moved
                    st[w, side, m] = dot(ct[g], moved).astype(BF16)
                    skp[q] = jnp.sum(gr * x_ref[:, part].astype(F32), axis=0, keepdims=True)

        def t_copy(w, k):
            m = pl.ds(width[w] * k, width[w])
            return remote(tt.at[w, m, 1 - half_of], t1.at[w, m], t1send.at[w, k], t1recv.at[w, k], in_pair)

        def u_copy(w, k):
            m = pl.ds(width[w] * k, width[w])
            return remote(us.at[w, m, 1 - pair], u2.at[w, m], u2send.at[w, k], u2recv.at[w, k], over_pairs)

        def v_copy(w, k):
            m = pl.ds(width[w] * k, width[w])
            return remote(vo.at[w, m], vi.at[w, m, pair], v2send.at[w, k], v2recv.at[w, k], over_pairs)

        def e_copy(w, k):
            m = pl.ds(width[w] * k, width[w])
            return remote(eo.at[w, m], er.at[w, m, half_of], e1send.at[w, k], e1recv.at[w, k], in_pair)

        def chip_decay(q, chip):
            return thx[q, pl.ds(2 * chip, 1), :] * thx[q, pl.ds(2 * chip + 1, 1), :]

        def pair_decay(q, which):
            return chip_decay(q, 2 * which) * chip_decay(q, 2 * which + 1)

        def chip_state(w, k):
            up, down = (0, 1) if w == 0 else (1, 0)
            partner_copy(w, k).wait_recv()
            for i in range(width[w]):
                m = width[w] * k + i
                own = st[w, mine, m].astype(F32)
                other = sp[w, m].astype(F32)
                first = jnp.where(c == up, own, other)
                second = jnp.where(c == up, other, own)
                decay = thx[quarter(m, mine), pl.ds(2 * y + down, 1), :]
                tt[w, m] = (decay * first + second).astype(BF16).reshape(2, 2 * ROWS, QL)
            t_copy(w, k).start()

        def pair_first(w, m):
            own = tt[w, m, half_of].astype(F32)
            other = t1[w, m].astype(F32)
            return jnp.where(low_y == w, own, other), jnp.where(low_y == w, other, own)

        def pair_step(w, k):
            t_copy(w, k).wait_recv()
            for i in range(width[w]):
                m = width[w] * k + i
                first, second = pair_first(w, m)
                decay = chip_decay(quarter(m, mine), 2 * pair + 1 - w)
                us[w, m] = (decay * first + second).astype(BF16).reshape(2, ROWS, QL)
            u_copy(w, k).start()

        def plane_first(w, m):
            own = us[w, m, pair].astype(F32)
            other = u2[w, m].astype(F32)
            return jnp.where(pair == w, own, other), jnp.where(pair == w, other, own)

        def chain_copy(k):
            m = pl.ds(width[0] * k, width[0])
            return remote(zs.at[m], zr.at[m], csend.at[k], crecv.at[k], z_peer(1))

        def across(k, other):
            m = pl.ds(width[1] * k, width[1])
            return remote(az.at[z, m], az.at[z, m], asend.at[k, other], arecv.at[k, z], (px, other, y, c))

        def down(k, other):
            m = pl.ds(width[1] * k, width[1])
            return remote(ho.at[m], hi.at[m], hsend.at[k, other], hrecv.at[k], (px, other, y, c))


        nearer = tuple(range(half // 2, half))
        farther = tuple(range(half // 2))

        def arrived(k, source):
            m = pl.ds(width[1] * k, width[1])
            return remote(az.at[source, m], az.at[source, m], asend.at[k, source], arecv.at[k, source], (px, source, y, c))

        def plane_total(w, m):
            q = quarter(m, mine)
            first, second = plane_first(w, m)
            decay = pair_decay(q, 1 - w)
            return decay * first + second, decay * pair_decay(q, w)

        def spread_out(w, k, values):
            for i, value in enumerate(values):
                m = width[w] * k + i
                after = pair_decay(quarter(m, mine), w) * value + plane_first(w, m)[0]
                vi[w, m, pair] = jnp.where(pair == w, value, after).astype(BF16)
                vo[w, m] = jnp.where(pair == w, after, value).astype(BF16)
            v_copy(w, k).start()

        def pair_out(w, k):
            v_copy(w, k).wait_recv()
            for i in range(width[w]):
                m = width[w] * k + i
                value = vi[w, m].reshape(2 * ROWS, QL).astype(F32)
                after = chip_decay(quarter(m, mine), 2 * pair + w) * value + pair_first(w, m)[0]
                er[w, m, half_of] = jnp.where(low_y == w, value, after).astype(BF16)
                eo[w, m] = jnp.where(low_y == w, after, value).astype(BF16)
            e_copy(w, k).start()

        def chain(k):
            u_copy(0, k).wait_recv()
            held = []
            for i in range(width[0]):
                m = width[0] * k + i
                total, factor = plane_total(0, m)
                tz_s[i] = total
                held.append((m, factor))

            @pl.when(z == 0)
            def _():
                for m, _factor in held:
                    zr[m] = jnp.zeros((ROWS, QL), BF16)

            @pl.when(z > 0)
            def _():
                chain_copy(k).wait_recv()

            @pl.when(z < nz - 1)
            def _():
                for i, (m, factor) in enumerate(held):
                    zs[m] = (factor * zr[m].astype(F32) + tz_s[i]).astype(BF16)
                chain_copy(k).start()

            spread_out(0, k, [zr[m].astype(F32) for m, _factor in held])

        def plane_send(k):
            u_copy(1, k).wait_recv()
            for i in range(width[1]):
                m = width[1] * k + i
                az[z, m] = plane_total(1, m)[0].astype(BF16)

            def body(other, carry):
                across(k, other).start()
                return carry

            lax.fori_loop(start, z, body, 0)

            @pl.when(to_top)
            def _():
                across(k, nz - 1).start()

        def hand_down(k, others):
            for i in range(width[1]):
                ho[width[1] * k + i] = tz_s[2 + i].astype(BF16)
            for other in others:
                down(k, other).start()

        def plane_back(k):
            @pl.when(z >= half)
            def _():
                for i in range(width[1]):
                    tz_s[i] = jnp.zeros((ROWS, QL), F32)

            @pl.when(z < half)
            def _():
                down(k, half).wait_recv()
                for i in range(width[1]):
                    tz_s[i] = hi[width[1] * k + i].astype(F32)

            def body(t, carry):
                source = start + half - 1 - t
                arrived(k, source).wait_recv()
                for i in range(width[1]):
                    m = width[1] * k + i
                    factor = fzx[quarter(m, mine), pl.ds(source, 1), :]
                    tz_s[i] = factor * tz_s[i] + az[source, m].astype(F32)
                return carry

            lax.fori_loop(0, start + half - 1 - z, body, 0)

            @pl.when(z == half)
            def _():
                for i in range(width[1]):
                    m = width[1] * k + i
                    total, factor = plane_total(1, m)
                    tz_s[2 + i] = factor * tz_s[i] + total
                hand_down(k, nearer)

            @pl.when(z == nz - 1)
            def _():
                for i in range(width[1]):
                    tz_s[2 + i] = plane_total(1, width[1] * k + i)[0]
                for t in range(half - 1):
                    source = nz - 2 - t
                    arrived(k, source).wait_recv()
                    for i in range(width[1]):
                        m = width[1] * k + i
                        factor = fzx[quarter(m, mine), source : source + 1, :]
                        tz_s[2 + i] = factor * tz_s[2 + i] + az[source, m].astype(F32)
                hand_down(k, farther)

            spread_out(1, k, [tz_s[i] for i in range(width[1])])

        def back_copy(w, k):
            return remote(some(epart, w, k), some(ex, w, k), psend.at[w, k], precv.at[w, k], (px, z, y, 1 - c))

        def hand_back(w, k):
            up = 0 if w == 0 else 1
            e_copy(w, k).wait_recv()
            for i in range(width[w]):
                m = width[w] * k + i
                here = er[w, m].reshape(N, QL).astype(F32)
                first = jnp.where(c == up, st[w, mine, m].astype(F32), sp[w, m].astype(F32))
                decay = thx[quarter(m, mine), pl.ds(2 * y + up, 1), :]
                after = decay * here + first
                keep[w, m] = jnp.where(c == up, here, after).astype(BF16)
                epart[w, m] = jnp.where(c == up, after, here).astype(BF16)
            back_copy(w, k).start()

        def finish_c(k):
            back_copy(0, k).wait_recv()
            for j in range(2):
                g = 2 * k + j
                acc = gca[g]
                for i in range(2):
                    m = 2 * g + i
                    acc = acc + dot_nt(gi[quarter(m, mine)], keep[0, m]) + dot_nt(gi[quarter(m, theirs)], ex[0, m])
                gc_out[:, lanes_of(g, N)] = acc.astype(BF16)

        def finish_b(g):
            back_copy(1, g).wait_recv()
            bg = b_ref[:, lanes_of(g, N)]
            acc = gba[g]
            for side, source in ((mine, keep), (theirs, ex)):
                for i in range(2):
                    m = 2 * g + i
                    q = quarter(m, side)
                    later = source[1, m]
                    acc = acc + dot_nt(xo[q], later)
                    gx_out[:, lanes_of(q, QL)] = (gxa[q] + lexp[q] * dot(bg, later)).astype(BF16)
            gb_out[:, lanes_of(g, N)] = acc.astype(BF16)

        def fwd_states(k, carry):
            states(0, k, theirs)
            partner_copy(0, k).start()
            states(0, k, mine)
            return carry

        lax.fori_loop(0, count[0], fwd_states, 0)

        for off in range(1, 2 * NY):
            info_copy(off).wait_recv()

        @pl.when(z > 0)
        def _():
            remote(info_s, info_r.at[2 * NY], isend.at[7], irecv.at[7], z_peer(nz - 1)).wait_recv()

        th_s[...] = jnp.zeros((16, H), F32)
        for i in range(2 * NY):
            before = info_r[2 * NY if i == 0 else i - 1, 1:2, :]
            th_s[i : i + 1, :] = jnp.exp(info_r[i, 0:1, :]) * jnp.where(info_r[i, 1:2, :] == before, 1.0, 0.0)
        th_s[8:9, :] = skip_ref[...]
        enter_from = info_r[lax.rem(d + 2 * NY, 2 * NY + 1), 1:2, :]
        segc = jnp.broadcast_to(seg_ref[...].astype(F32), (T, T)).T
        enter = jnp.exp(cum_s[...]) * jnp.where(segc == enter_from, 1.0, 0.0)
        lvs[...] = jnp.concatenate(split(enter, 2), axis=1)
        whole = th_s[0:1, :]
        for i in range(1, 2 * NY):
            whole = whole * th_s[i : i + 1, :]
        fz_s[...] = jnp.broadcast_to(whole, (8, H))
        fz_r[z] = fz_s[...]

        def f_copy(other):
            return remote(fz_s, fz_r.at[z], fsend.at[other], frecv.at[z], (px, other, y, c))

        def f_arrived(source):
            return remote(fz_s, fz_r.at[source], fsend.at[source], frecv.at[source], (px, source, y, c))

        def f_start(other, carry):
            f_copy(other).start()
            return carry

        lax.fori_loop(0, z, f_start, 0)
        @pl.when(to_top)
        def _():
            f_copy(nz - 1).start()


        def table(k, carry):
            rows = jnp.concatenate(split(th_s[...], 3), axis=1)
            for i in range(4):
                thx[4 * k + i] = dot(rows, indicator(4 * k + i, 3))
            return carry

        lax.fori_loop(0, QUARTERS // 4, table, 0)

        def fwd_chip(k, carry):
            chip_state(0, k)
            return carry

        lax.fori_loop(0, count[0], fwd_chip, 0)

        def enter_wide(k, carry):
            for i in range(4):
                eexp[4 * k + i] = dot(lvs[...], indicator(4 * k + i, 2))
            return carry

        enter_wide(0, 0)

        def f_wait(t, carry):
            f_arrived(nz - 1 - t).wait_recv()
            return carry

        def plane_table():
            lax.fori_loop(0, nz - 1 - z, f_wait, 0)

            @pl.when(z == nz - 1)
            def _():
                for source in range(half, nz - 1):
                    f_arrived(source).wait_recv()

            everything = jnp.concatenate(
                [
                    jnp.where((i > z) | (z == nz - 1 if half <= i < nz - 1 else False), fz_r[i, 0:1, :], 0.0)
                    for i in range(nz)
                ],
                axis=0,
            )
            th_s[0:nz, :] = everything

            def body(k, carry):
                rows = jnp.concatenate(split(th_s[...], 3), axis=1)
                for i in range(4):
                    fzx[4 * k + i] = dot(rows, indicator(4 * k + i, 3))
                return carry

            lax.fori_loop(0, QUARTERS // 4, body, 0)

        def within(g):
            bg = b_ref[:, lanes_of(g, N)]
            cg = c_ref[:, lanes_of(g, N)]
            cross = dot_nt(bg, cg)
            cols = pltpu.roll(cum_s[...], lax.rem(H - 16 * g, H), 1)
            low = lax.broadcasted_iota(jnp.int32, (T, T), 1) < D
            total = jnp.zeros((T, T), F32)
            for j in range(8):
                part = pl.ds(pl.multiple_of(1024 * g + 128 * j, 128), 128)
                gf = grad[:, part].astype(F32)
                xp = x_ref[:, part]
                both = jnp.concatenate(
                    [jnp.where(low, gf, 0.0).astype(BF16), jnp.where(low, 0.0, gf).astype(BF16)], axis=0
                )
                prod = dot_nt(both, xp)
                pieces = []
                for i in range(2):
                    j2 = 2 * j + i
                    spread = cols[:, j2 : j2 + 1] - cumt_s[pl.ds(16 * g + j2, 1), :]
                    total = total + jnp.exp(spread + bias_s[...]) * prod[T * i : T * i + T, :]
                    pieces.append((jnp.exp(biast_s[...] - spread) * cross).astype(BF16))
                out = dot(jnp.concatenate(pieces, axis=1), both)
                half = slice(128 * (j % 2), 128 * (j % 2) + 128)
                q = 4 * g + j // 2
                gxa[q, :, half] = out + thx[q, 8:9, half] * gf
            gca[g] = dot(total.astype(BF16), bg)
            gba[g] = dot(total.T.astype(BF16), cg)

        def sk_copy(off):
            return remote(sk_s, sk_r.at[d], ssend.at[off - 1], srecv.at[off - 1], plane_peer(off))

        def skz_copy(off):
            return remote(skz_s, skz_r.at[z], zsend.at[off - 1], zrecv.at[off - 1], z_peer(off))

        def sk_plane():
            row_q = lax.broadcasted_iota(jnp.int32, (QL, 128), 0)
            col_q = lax.broadcasted_iota(jnp.int32, (QL, 128), 1)
            pick = jnp.where(lax.shift_right_logical(row_q, 6) == (col_q & 3), 1.0, 0.0).astype(BF16)
            sums = jnp.reshape(skp[...], (QUARTERS, QL))
            heads = sum(dot(piece, pick) for piece in split(sums, 3))
            own_row = lax.broadcasted_iota(jnp.int32, (QUARTERS, 128), 0)
            own_col = lax.broadcasted_iota(jnp.int32, (QUARTERS, 128), 1)
            heads = jnp.where(lax.shift_right_logical(own_col, 2) == own_row, heads, 0.0)
            sk_s[...] = jnp.broadcast_to(jnp.sum(heads, axis=0, keepdims=True), (8, 128))
            sk_r[d] = sk_s[...]
            for off in range(1, 2 * NY):
                sk_copy(off).start()

        def sk_along():
            for off in range(1, 2 * NY):
                sk_copy(off).wait_recv()
            acc = sk_r[0]
            for i in range(1, 2 * NY):
                acc = acc + sk_r[i]
            skz_s[...] = acc
            skz_r[z] = acc
            for off in range(1, nz):
                skz_copy(off).start()

        def each(n, step):
            def body(k, carry):
                step(k)
                return carry

            lax.fori_loop(0, n, body, 0)

        chain_at = 2 + lax.div(z * 5 + 3, nz - 1)
        back_at = jnp.where(z < half, 4, 3)

        def main(k, carry):
            def at(lag, n, step):
                @pl.when((k >= lag) & (k < lag + n))
                def _():
                    step(k - lag)

            def begin(k):
                @pl.when(px == nx - 1)
                def _():
                    for i in range(4):
                        part = lanes_of(4 * k + i, QL)
                        grad[:, part] = (grad[:, part].astype(F32) * wide_s[...]).astype(BF16)

                @pl.when(px < nx - 1)
                def _():
                    grad_copy(k).wait_recv()

                states(1, k, theirs)
                partner_copy(1, k).start()
                states(1, k, mine)

                @pl.when(k < CHUNKS - 1)
                def _():
                    enter_wide(k + 1, 0)

                chip_state(1, k)
                within(k)

            at(0, CHUNKS, begin)

            @pl.when(k == 1)
            def _():
                plane_table()

            def at_pairing_end(lag, n, step):
                @pl.when((k >= lag) & (k < lag + n - 1))
                def _():
                    step(k - lag)

                @pl.when(k == lag + n - 2)
                def _():
                    step(k - lag + 1)

            def two(step):
                def both(i):
                    step(2 * i)
                    step(2 * i + 1)

                return both

            at(1, count[1] - 1, lambda i: pair_step(1, i))
            at(2, count[1] - 2, plane_send)

            @pl.when(k == CHUNKS)
            def _():
                plane_send(CHUNKS - 1)
                sk_plane()

            at_pairing_end(back_at, count[1], plane_back)

            @pl.when(k == CHUNKS - 1)
            def _():
                pair_step(1, k)
                plane_send(k - 1)

            at_pairing_end(back_at + 1, count[1], lambda i: pair_out(1, i))
            at_pairing_end(back_at + 2, count[1], lambda i: hand_back(1, i))

            @pl.when(k == CHUNKS + 2)
            def _():
                sk_along()

            at_pairing_end(back_at + 3, count[1], finish_b)
            at(1, count[0] // 2, two(lambda i: pair_step(0, i)))

            @pl.when(z < nz - 1)
            def _():
                at(chain_at + 1, count[0], lambda i: pair_out(0, i))

            @pl.when(z == nz - 1)
            def _():
                at(chain_at + 1, count[0] // 2, two(lambda i: pair_out(0, i)))

            at(chain_at, count[0] // 2, two(chain))

            @pl.when(z < nz - 1)
            def _():
                at(chain_at + 2, count[0], lambda i: hand_back(0, i))

            @pl.when(z == nz - 1)
            def _():
                at(chain_at + 2, count[0] // 2, two(lambda i: hand_back(0, i)))

            at(chain_at + 3, count[0], finish_c)
            return carry

        lax.fori_loop(0, CHUNKS + 6, main, 0)

        for off in range(1, nz):
            skz_copy(off).wait_recv()
        acc = skz_r[0]
        for i in range(1, nz):
            acc = acc + skz_r[i]
        sk_out[...] = acc[0:1, :]

        @pl.when(px > 0)
        def _():
            def body(k, carry):
                grad_copy(k).wait_send()
                return carry

            lax.fori_loop(0, CHUNKS, body, 0)

        for off in range(1, 2 * NY):
            info_copy(off).wait_send()
            sk_copy(off).wait_send()

        @pl.when((d == last_d) & (z < nz - 1))
        def _():
            for other in range(2 * NY):
                info_next(other).wait_send()

        for off in range(1, nz):
            skz_copy(off).wait_send()

        for w in range(2):

            def drain(k, w=w):
                partner_copy(w, k).wait_send()
                back_copy(w, k).wait_send()
                t_copy(w, k).wait_send()
                u_copy(w, k).wait_send()
                v_copy(w, k).wait_send()
                e_copy(w, k).wait_send()
                if w == 0:

                    @pl.when(z < nz - 1)
                    def _():
                        chain_copy(k).wait_send()
                else:

                    def let_go(other, carry, k=k):
                        across(k, other).wait_send()
                        return carry

                    lax.fori_loop(start, z, let_go, 0)

                    @pl.when(to_top)
                    def _(k=k):
                        across(k, nz - 1).wait_send()

                    @pl.when(z == half)
                    def _(k=k):
                        for other in nearer:
                            down(k, other).wait_send()

                    @pl.when(z == nz - 1)
                    def _(k=k):
                        for other in farther:
                            down(k, other).wait_send()


            each(count[w], drain)
        each(z, lambda other: f_copy(other).wait_send())

        @pl.when(to_top)
        def _():
            f_copy(nz - 1).wait_send()


    return kernel


def call(nx, nz):
    vm = pltpu.VMEM
    dma = pltpu.SemaphoreType.DMA
    scratch = [
        vm((T, H * D), BF16),
        vm((T, GROUPS * N), BF16),
        vm((T, GROUPS * N), BF16),
        vm((T, H), F32),
        dma((5,)),
        vm((T, H * D), BF16),
        vm((QUARTERS, T, QL), BF16),
        vm((QUARTERS, T, QL), BF16),
        vm((QUARTERS, T, QL), F32),
        vm((QUARTERS, T, QL), F32),
        vm((GROUPS, T, N), F32),
        vm((GROUPS, T, N), F32),
        vm((T, H), F32),
        vm((H, T), F32),
        vm((T, T), F32),
        vm((T, T), F32),
        vm((QUARTERS, T, QL), F32),
        vm((T, 2 * H), BF16),
        vm((GROUPS, N, T), BF16),
        vm((GROUPS, N, T), BF16),
        vm((T, QL), F32),
        vm((8, H), F32),
        vm((nz, 8, H), F32),
        vm((QUARTERS, 16, QL), F32),
        vm((8, H), F32),
        vm((2 * NY + 1, 8, H), F32),
        vm((16, H), F32),
        vm((QUARTERS, 16, QL), F32),
        vm((2, 2, MINE, N, QL), BF16),
        vm((2, MINE, N, QL), BF16),
        vm((2, MINE, 2, 2 * ROWS, QL), BF16),
        vm((2, MINE, 2 * ROWS, QL), BF16),
        vm((2, MINE, 2, ROWS, QL), BF16),
        vm((2, MINE, ROWS, QL), BF16),
        vm((MINE, ROWS, QL), BF16),
        vm((MINE, ROWS, QL), BF16),
        vm((nz, MINE, ROWS, QL), BF16),
        vm((MINE, ROWS, QL), BF16),
        vm((MINE, ROWS, QL), BF16),
        vm((2, MINE, ROWS, QL), BF16),
        vm((2, MINE, 2, ROWS, QL), BF16),
        vm((2, MINE, 2 * ROWS, QL), BF16),
        vm((2, MINE, 2, 2 * ROWS, QL), BF16),
        vm((2, MINE, N, QL), BF16),
        vm((2, MINE, N, QL), BF16),
        vm((2, MINE, N, QL), BF16),
        vm((4, ROWS, QL), F32),
        vm((QUARTERS, 1, QL), F32),
        vm((8, 128), F32),
        vm((2 * NY, 8, 128), F32),
        vm((8, 128), F32),
        vm((nz, 8, 128), F32),
        dma((CHUNKS,)), dma((CHUNKS,)),
        dma((7 + 2 * NY,)), dma((8,)),
        dma((7,)), dma((7,)),
        dma((nz - 1,)), dma((nz - 1,)),
        dma((nz,)), dma((nz,)),
        dma((CHUNKS, nz)), dma((CHUNKS, nz)),
        dma((CHUNKS, nz)), dma((CHUNKS,)),
        dma((2, CHUNKS)), dma((2, CHUNKS)),
        dma((2, CHUNKS)), dma((2, CHUNKS)),
        dma((2, CHUNKS)), dma((2, CHUNKS)),
        dma((MINE // 4,)), dma((MINE // 4,)),
        dma((2, CHUNKS)), dma((2, CHUNKS)),
        dma((2, CHUNKS)), dma((2, CHUNKS)),
        dma((2, CHUNKS)), dma((2, CHUNKS)),
    ]
    return pl.pallas_call(
        make_kernel(nx, nz),
        out_shape=(
            vm((T, H * D), BF16),
            vm((T, GROUPS * N), BF16),
            vm((T, GROUPS * N), BF16),
            vm((1, H), F32),
        ),
        in_specs=[pl.BlockSpec(memory_space=pl.ANY)] * 5 + [pl.BlockSpec(memory_space=pltpu.VMEM)] * 4,
        out_specs=[pl.BlockSpec(memory_space=pltpu.VMEM)] * 4,
        scratch_shapes=scratch,
        compiler_params=pltpu.CompilerParams(vmem_limit_bytes=56 * 2**20, collective_id=0, has_side_effects=True),
        name="mixer_backward",
    )


def deliver(*results):
    def kernel(*refs):
        n = len(results)
        sem = refs[2 * n]
        copies = [pltpu.make_async_copy(refs[i], refs[n + i], sem.at[i]) for i in range(n)]
        for copy in copies:
            copy.start()
        for copy in copies:
            copy.wait()

    return pl.pallas_call(
        kernel,
        out_shape=tuple(jax.ShapeDtypeStruct(v.shape, v.dtype) for v in results),
        in_specs=[pl.BlockSpec(memory_space=pltpu.VMEM)] * len(results),
        out_specs=[pl.BlockSpec(memory_space=pl.ANY)] * len(results),
        scratch_shapes=[pltpu.SemaphoreType.DMA((len(results),))],
        compiler_params=pltpu.CompilerParams(vmem_limit_bytes=2**20),
        name="deliver",
    )(*results)


def on_device(previous, saved_head_inputs, input_b, input_c, steps, decay_rate, skip_gain, segment_ids, advantage_mask):
    kernel = call(lax.axis_size("pipe"), lax.axis_size("seq_0"))
    gx, gb, gc, sk = kernel(
        previous[0],
        saved_head_inputs[0],
        input_b[0],
        input_c[0],
        steps[0],
        decay_rate,
        skip_gain,
        segment_ids,
        advantage_mask[None],
    )
    gx, gb, gc, sk = deliver(gx, gb, gc, sk)
    return gx[None], gb[None], gc[None], sk


def solution(mesh):
    finer = Mesh(
        mesh.devices.reshape(mesh.shape["pipe"], mesh.shape["seq"] // (2 * NY), NY, 2),
        ("pipe", "seq_0", "seq_1", "seq_2"),
    )
    return jax.shard_map(
        on_device,
        mesh=finer,
        in_specs=(
            P("pipe", SEQ, None),
            P("pipe", SEQ, None),
            P("pipe", SEQ, None),
            P("pipe", SEQ, None),
            P("pipe", SEQ, None),
            P("pipe", None),
            P("pipe", None),
            P("pipe", SEQ),
            P(SEQ),
        ),
        out_specs=(
            P("pipe", SEQ, None),
            P("pipe", SEQ, None),
            P("pipe", SEQ, None),
            P("pipe", None),
        ),
        check_vma=False,
    )
```

```python
import jax
import jax.numpy as jnp
from jax import lax
from jax.experimental import pallas as pl
from jax.experimental.pallas import tpu as pltpu
from jax.sharding import Mesh
from jax.sharding import PartitionSpec as P

SEQ = ("seq_0", "seq_1", "seq_2")
MESH = pl.DeviceIdType.MESH
F32 = jnp.float32
BF16 = jnp.bfloat16
NY = 4
T = 128
N = 128
H = 128
D = 64
GROUPS = 8
CHUNKS = 8
MINE = 2 * CHUNKS
ROWS = N // NY
QL = 256
QUARTERS = 32


def split(v, parts):
    out = []
    for _ in range(parts):
        piece = v.astype(BF16)
        out.append(piece)
        v = v - piece.astype(F32)
    return out


def dot(a, b):
    return lax.dot_general(a, b, (((1,), (0,)), ((), ())), preferred_element_type=F32)


def dot_nt(a, b):
    return lax.dot_general(a, b, (((1,), (1,)), ((), ())), preferred_element_type=F32)


def lanes_of(index, width):
    return pl.ds(pl.multiple_of(index * width, width), width)


def indicator(q, copies):
    row = lax.broadcasted_iota(jnp.int32, (H, QL), 0)
    col = lax.broadcasted_iota(jnp.int32, (H, QL), 1)
    one = jnp.where(row == 4 * q + lax.shift_right_logical(col, 6), 1.0, 0.0).astype(BF16)
    return jnp.concatenate([one] * copies, axis=0)


def make_kernel(nx, nz):
    width = (4, 2)
    count = (MINE // 4, CHUNKS)

    def kernel(
        prev_ref, x_hbm, b_hbm, c_hbm, steps_hbm, rate_ref, skip_ref, seg_ref, mask_ref,
        gx_out, gb_out, gc_out, sk_out,
        x_ref, b_ref, c_ref, steps_ref, lsem,
        grad, xo, gi, gxa, lexp, gca, gba, cum_s, cumt_s, bias_s, biast_s, eexp, lvs, ens, bt, ct, wide_s, fz_s, fz_r, fzx,
        info_s, info_r, th_s, thx,
        st, sp, tt, t1, us, u2, zs, zr, az, ho, hi, vo, vi, eo, er, keep, epart, ex, tz_s,
        skp, sk_s, sk_r, skz_s, skz_r,
        gsend, grecv, isend, irecv, ssend, srecv, zsend, zrecv,
        fsend, frecv, asend, arecv, hsend, hrecv, dsend, drecv, t1send, t1recv, u2send, u2recv, csend, crecv, v2send, v2recv, e1send, e1recv, psend, precv,
    ):
        px = lax.axis_index("pipe")
        z = lax.axis_index("seq_0")
        y = lax.axis_index("seq_1")
        c = lax.axis_index("seq_2")
        d = 2 * y + c
        last_d = 2 * NY - 1
        half = nz // 2
        start = half * lax.div(z, half)
        to_top = (z >= half) & (z < nz - 1)

        def remote(src, dst, ssem, rsem, where):
            return pltpu.make_async_remote_copy(
                src_ref=src, dst_ref=dst, send_sem=ssem, recv_sem=rsem, device_id=where, device_id_type=MESH
            )

        def plane_peer(off):
            other = lax.rem(d + off, 2 * NY)
            return (px, z, lax.div(other, 2), lax.rem(other, 2))

        def z_peer(off):
            return (px, lax.rem(z + off, nz), y, c)

        loads = [
            pltpu.make_async_copy(src, dst, lsem.at[i])
            for i, (src, dst) in enumerate(
                ((steps_hbm, steps_ref), (b_hbm, b_ref), (c_hbm, c_ref), (x_hbm, x_ref), (prev_ref, grad))
            )
        ]
        for load in loads[:4]:
            load.start()

        @pl.when(px == nx - 1)
        def _():
            loads[4].start()

        barrier = pltpu.get_barrier_semaphore()

        def greet(where):
            pl.semaphore_signal(barrier, inc=1, device_id=where, device_id_type=MESH)

        for off in range(1, 2 * NY):
            greet(plane_peer(off))
        for off in range(1, nz):
            greet(z_peer(off))

        @pl.when(px < nx - 1)
        def _():
            greet((lax.rem(px + 1, nx), z, y, c))

        @pl.when(z > 0)
        def _():
            greet((px, lax.rem(z + nz - 1, nz), NY - 1, 1))

        from_next = (d == last_d) & (z < nz - 1)
        callers = 2 * NY - 1 + nz - 1 + jnp.where(px > 0, 1, 0) + jnp.where(from_next, 2 * NY, 0)
        pl.semaphore_wait(barrier, callers)

        def grad_copy(k):
            part = lanes_of(k, 4 * QL)
            return remote(
                prev_ref.at[:, part], grad.at[:, part], gsend.at[k], grecv.at[k], (lax.rem(px + nx - 1, nx), z, y, c)
            )

        @pl.when(px > 0)
        def _():
            def body(k, carry):
                grad_copy(k).start()
                return carry

            lax.fori_loop(0, CHUNKS, body, 0)

        row = lax.broadcasted_iota(jnp.int32, (T, T), 0)
        col = lax.broadcasted_iota(jnp.int32, (T, T), 1)
        loads[0].wait()
        cum = -(steps_ref[...] * rate_ref[...])
        for shift in (1, 2, 4, 8, 16, 32, 64):
            cum = cum + jnp.where(row >= shift, pltpu.roll(cum, shift, 0), 0.0)
        cum_s[...] = cum
        cumt_s[...] = cum.T
        last = cum[T - 1 : T, :]
        segrow = jnp.broadcast_to(seg_ref[...].astype(F32), (T, T))
        segcol = segrow.T
        seglast = segcol[T - 1 : T, :]
        info_s[0:1, :] = last
        info_s[1:2, :] = seglast
        info_s[2:8, :] = jnp.zeros((6, H), F32)
        info_r[d] = info_s[...]

        def info_copy(off):
            return remote(info_s, info_r.at[d], isend.at[off - 1], irecv.at[off - 1], plane_peer(off))

        def info_next(other):
            return remote(
                info_s, info_r.at[2 * NY], isend.at[7 + other], irecv.at[7], (px, lax.rem(z + 1, nz), other // 2, other % 2)
            )

        for off in range(1, 2 * NY):
            info_copy(off).start()

        @pl.when((d == last_d) & (z < nz - 1))
        def _():
            for other in range(2 * NY):
                info_next(other).start()

        @pl.when(z == 0)
        def _():
            info_r[2 * NY] = jnp.full((8, H), -1.0, F32)

        linked = segcol == segrow
        bias_s[...] = jnp.where(linked & (row >= col), 0.0, -1e30)
        biast_s[...] = jnp.where(linked & (col >= row), 0.0, -1e30)
        leave = jnp.exp(last - cum) * jnp.where(segcol == seglast, 1.0, 0.0)
        lvs[...] = jnp.concatenate(split(leave, 2), axis=1)
        kept = jnp.broadcast_to(mask_ref[...].astype(F32), (T, T)).T
        wide_s[...] = jnp.concatenate([kept, kept], axis=1)

        for load in loads[1:4]:
            load.wait()

        @pl.when(px == nx - 1)
        def _():
            loads[4].wait()

        for g in range(GROUPS):
            part = slice(N * g, N * g + N)
            bt[g] = b_ref[:, part].astype(F32).T.astype(BF16)
            ct[g] = c_ref[:, part].astype(F32).T.astype(BF16)

        pair = lax.div(y, 2)
        low_y = lax.rem(y, 2)
        half_of = jnp.where(low_y == pair, 0, 1)
        in_pair = (px, z, 2 * pair + 1 - low_y, c)
        over_pairs = (px, z, NY - 1 - y, c)

        mine = c
        theirs = 1 - c

        def some(ref, w, k):
            return ref.at[w, pl.ds(width[w] * k, width[w])]

        def partner_copy(w, k):
            n = width[w]
            return remote(
                st.at[w, theirs, pl.ds(n * k, n)], some(sp, w, k), dsend.at[w, k], drecv.at[w, k], (px, z, y, 1 - c)
            )

        def quarter(m, side):
            return 4 * lax.div(m, 2) + 2 * side + lax.rem(m, 2)

        def states(w, k, side):
            for i in range(width[w]):
                m = width[w] * k + i
                q = quarter(m, side)
                g = lax.div(m, 2)
                part = lanes_of(q, QL)
                if w == 0:
                    factor = dot(lvs[...], indicator(q, 2))
                    lexp[q] = factor
                    moved = (factor * x_ref[:, part].astype(F32)).astype(BF16)
                    xo[q] = moved
                    st[w, side, m] = dot(bt[g], moved).astype(BF16)
                else:
                    gr = grad[:, part].astype(F32)
                    moved = (eexp[q] * gr).astype(BF16)
                    gi[q] = moved
                    st[w, side, m] = dot(ct[g], moved).astype(BF16)
                    skp[q] = jnp.sum(gr * x_ref[:, part].astype(F32), axis=0, keepdims=True)

        def t_copy(w, k):
            m = pl.ds(width[w] * k, width[w])
            return remote(tt.at[w, m, 1 - half_of], t1.at[w, m], t1send.at[w, k], t1recv.at[w, k], in_pair)

        def u_copy(w, k):
            m = pl.ds(width[w] * k, width[w])
            return remote(us.at[w, m, 1 - pair], u2.at[w, m], u2send.at[w, k], u2recv.at[w, k], over_pairs)

        def v_copy(w, k):
            m = pl.ds(width[w] * k, width[w])
            return remote(vo.at[w, m], vi.at[w, m, pair], v2send.at[w, k], v2recv.at[w, k], over_pairs)

        def e_copy(w, k):
            m = pl.ds(width[w] * k, width[w])
            return remote(eo.at[w, m], er.at[w, m, half_of], e1send.at[w, k], e1recv.at[w, k], in_pair)

        def chip_decay(q, chip):
            return thx[q, pl.ds(2 * chip, 1), :] * thx[q, pl.ds(2 * chip + 1, 1), :]

        def pair_decay(q, which):
            return chip_decay(q, 2 * which) * chip_decay(q, 2 * which + 1)

        def chip_state(w, k):
            up, down = (0, 1) if w == 0 else (1, 0)
            partner_copy(w, k).wait_recv()
            for i in range(width[w]):
                m = width[w] * k + i
                own = st[w, mine, m].astype(F32)
                other = sp[w, m].astype(F32)
                first = jnp.where(c == up, own, other)
                second = jnp.where(c == up, other, own)
                decay = thx[quarter(m, mine), pl.ds(2 * y + down, 1), :]
                tt[w, m] = (decay * first + second).astype(BF16).reshape(2, 2 * ROWS, QL)
            t_copy(w, k).start()

        def pair_first(w, m):
            own = tt[w, m, half_of].astype(F32)
            other = t1[w, m].astype(F32)
            return jnp.where(low_y == w, own, other), jnp.where(low_y == w, other, own)

        def pair_step(w, k):
            t_copy(w, k).wait_recv()
            for i in range(width[w]):
                m = width[w] * k + i
                first, second = pair_first(w, m)
                decay = chip_decay(quarter(m, mine), 2 * pair + 1 - w)
                us[w, m] = (decay * first + second).astype(BF16).reshape(2, ROWS, QL)
            u_copy(w, k).start()

        def plane_first(w, m):
            own = us[w, m, pair].astype(F32)
            other = u2[w, m].astype(F32)
            return jnp.where(pair == w, own, other), jnp.where(pair == w, other, own)

        def chain_copy(k):
            m = pl.ds(width[0] * k, width[0])
            return remote(zs.at[m], zr.at[m], csend.at[k], crecv.at[k], z_peer(1))

        def across(k, other):
            m = pl.ds(width[1] * k, width[1])
            return remote(az.at[z, m], az.at[z, m], asend.at[k, other], arecv.at[k, z], (px, other, y, c))

        def down(k, other):
            m = pl.ds(width[1] * k, width[1])
            return remote(ho.at[m], hi.at[m], hsend.at[k, other], hrecv.at[k], (px, other, y, c))


        nearer = tuple(range(half // 2, half))
        farther = tuple(range(half // 2))

        def arrived(k, source):
            m = pl.ds(width[1] * k, width[1])
            return remote(az.at[source, m], az.at[source, m], asend.at[k, source], arecv.at[k, source], (px, source, y, c))

        def plane_total(w, m):
            q = quarter(m, mine)
            first, second = plane_first(w, m)
            decay = pair_decay(q, 1 - w)
            return decay * first + second, decay * pair_decay(q, w)

        def spread_out(w, k, values):
            for i, value in enumerate(values):
                m = width[w] * k + i
                after = pair_decay(quarter(m, mine), w) * value + plane_first(w, m)[0]
                vi[w, m, pair] = jnp.where(pair == w, value, after).astype(BF16)
                vo[w, m] = jnp.where(pair == w, after, value).astype(BF16)
            v_copy(w, k).start()

        def pair_out(w, k):
            v_copy(w, k).wait_recv()
            for i in range(width[w]):
                m = width[w] * k + i
                value = vi[w, m].reshape(2 * ROWS, QL).astype(F32)
                after = chip_decay(quarter(m, mine), 2 * pair + w) * value + pair_first(w, m)[0]
                er[w, m, half_of] = jnp.where(low_y == w, value, after).astype(BF16)
                eo[w, m] = jnp.where(low_y == w, after, value).astype(BF16)
            e_copy(w, k).start()

        def chain(k):
            u_copy(0, k).wait_recv()
            held = []
            for i in range(width[0]):
                m = width[0] * k + i
                total, factor = plane_total(0, m)
                tz_s[i] = total
                held.append((m, factor))

            @pl.when(z == 0)
            def _():
                for m, _factor in held:
                    zr[m] = jnp.zeros((ROWS, QL), BF16)

            @pl.when(z > 0)
            def _():
                chain_copy(k).wait_recv()

            @pl.when(z < nz - 1)
            def _():
                for i, (m, factor) in enumerate(held):
                    zs[m] = (factor * zr[m].astype(F32) + tz_s[i]).astype(BF16)
                chain_copy(k).start()

            spread_out(0, k, [zr[m].astype(F32) for m, _factor in held])

        def plane_send(k):
            u_copy(1, k).wait_recv()
            for i in range(width[1]):
                m = width[1] * k + i
                az[z, m] = plane_total(1, m)[0].astype(BF16)

            def body(other, carry):
                across(k, other).start()
                return carry

            lax.fori_loop(start, z, body, 0)

            @pl.when(to_top)
            def _():
                across(k, nz - 1).start()

        def hand_down(k, others):
            for i in range(width[1]):
                ho[width[1] * k + i] = tz_s[2 + i].astype(BF16)
            for other in others:
                down(k, other).start()

        def plane_back(k):
            @pl.when(z >= half)
            def _():
                for i in range(width[1]):
                    tz_s[i] = jnp.zeros((ROWS, QL), F32)

            @pl.when(z < half)
            def _():
                down(k, half).wait_recv()
                for i in range(width[1]):
                    tz_s[i] = hi[width[1] * k + i].astype(F32)

            def body(t, carry):
                source = start + half - 1 - t
                arrived(k, source).wait_recv()
                for i in range(width[1]):
                    m = width[1] * k + i
                    factor = fzx[quarter(m, mine), pl.ds(source, 1), :]
                    tz_s[i] = factor * tz_s[i] + az[source, m].astype(F32)
                return carry

            lax.fori_loop(0, start + half - 1 - z, body, 0)

            @pl.when(z == half)
            def _():
                for i in range(width[1]):
                    m = width[1] * k + i
                    total, factor = plane_total(1, m)
                    tz_s[2 + i] = factor * tz_s[i] + total
                hand_down(k, nearer)

            @pl.when(z == nz - 1)
            def _():
                for i in range(width[1]):
                    tz_s[2 + i] = plane_total(1, width[1] * k + i)[0]
                for t in range(half - 1):
                    source = nz - 2 - t
                    arrived(k, source).wait_recv()
                    for i in range(width[1]):
                        m = width[1] * k + i
                        factor = fzx[quarter(m, mine), source : source + 1, :]
                        tz_s[2 + i] = factor * tz_s[2 + i] + az[source, m].astype(F32)
                hand_down(k, farther)

            spread_out(1, k, [tz_s[i] for i in range(width[1])])

        def back_copy(w, k):
            return remote(some(epart, w, k), some(ex, w, k), psend.at[w, k], precv.at[w, k], (px, z, y, 1 - c))

        def hand_back(w, k):
            up = 0 if w == 0 else 1
            e_copy(w, k).wait_recv()
            for i in range(width[w]):
                m = width[w] * k + i
                here = er[w, m].reshape(N, QL).astype(F32)
                first = jnp.where(c == up, st[w, mine, m].astype(F32), sp[w, m].astype(F32))
                decay = thx[quarter(m, mine), pl.ds(2 * y + up, 1), :]
                after = decay * here + first
                keep[w, m] = jnp.where(c == up, here, after).astype(BF16)
                epart[w, m] = jnp.where(c == up, after, here).astype(BF16)
            back_copy(w, k).start()

        def finish_c(k):
            back_copy(0, k).wait_recv()
            for j in range(2):
                g = 2 * k + j
                acc = gca[g]
                for i in range(2):
                    m = 2 * g + i
                    acc = acc + dot_nt(gi[quarter(m, mine)], keep[0, m]) + dot_nt(gi[quarter(m, theirs)], ex[0, m])
                gc_out[:, lanes_of(g, N)] = acc.astype(BF16)

        def finish_b(g):
            back_copy(1, g).wait_recv()
            bg = b_ref[:, lanes_of(g, N)]
            acc = gba[g]
            for side, source in ((mine, keep), (theirs, ex)):
                for i in range(2):
                    m = 2 * g + i
                    q = quarter(m, side)
                    later = source[1, m]
                    acc = acc + dot_nt(xo[q], later)
                    gx_out[:, lanes_of(q, QL)] = (gxa[q] + lexp[q] * dot(bg, later)).astype(BF16)
            gb_out[:, lanes_of(g, N)] = acc.astype(BF16)

        def fwd_states(k, carry):
            states(0, k, theirs)
            partner_copy(0, k).start()
            states(0, k, mine)
            return carry

        lax.fori_loop(0, count[0] // 2, fwd_states, 0)

        for off in range(1, 2 * NY):
            info_copy(off).wait_recv()

        @pl.when(z > 0)
        def _():
            remote(info_s, info_r.at[2 * NY], isend.at[7], irecv.at[7], z_peer(nz - 1)).wait_recv()

        th_s[...] = jnp.zeros((16, H), F32)
        for i in range(2 * NY):
            before = info_r[2 * NY if i == 0 else i - 1, 1:2, :]
            th_s[i : i + 1, :] = jnp.exp(info_r[i, 0:1, :]) * jnp.where(info_r[i, 1:2, :] == before, 1.0, 0.0)
        th_s[8:9, :] = skip_ref[...]
        enter_from = info_r[lax.rem(d + 2 * NY, 2 * NY + 1), 1:2, :]
        segc = jnp.broadcast_to(seg_ref[...].astype(F32), (T, T)).T
        enter = jnp.exp(cum_s[...]) * jnp.where(segc == enter_from, 1.0, 0.0)
        whole = th_s[0:1, :]
        for i in range(1, 2 * NY):
            whole = whole * th_s[i : i + 1, :]
        fz_s[...] = jnp.broadcast_to(whole, (8, H))
        fz_r[z] = fz_s[...]

        def f_copy(other):
            return remote(fz_s, fz_r.at[z], fsend.at[other], frecv.at[z], (px, other, y, c))

        def f_arrived(source):
            return remote(fz_s, fz_r.at[source], fsend.at[source], frecv.at[source], (px, source, y, c))

        def f_start(other, carry):
            f_copy(other).start()
            return carry

        lax.fori_loop(0, z, f_start, 0)
        @pl.when(to_top)
        def _():
            f_copy(nz - 1).start()


        def table(k, carry):
            rows = jnp.concatenate(split(th_s[...], 3), axis=1)
            for i in range(4):
                thx[4 * k + i] = dot(rows, indicator(4 * k + i, 3))
            return carry

        lax.fori_loop(0, QUARTERS // 4, table, 0)
        ens[...] = jnp.concatenate(split(enter, 2), axis=1)

        def fwd_chip(k, carry):
            chip_state(0, k)
            return carry

        lax.fori_loop(0, count[0] // 2, fwd_chip, 0)

        def enter_wide(k, carry):
            for i in range(4):
                eexp[4 * k + i] = dot(ens[...], indicator(4 * k + i, 2))
            return carry

        enter_wide(0, 0)
        lax.fori_loop(count[0] // 2, count[0], fwd_states, 0)
        lax.fori_loop(count[0] // 2, count[0], fwd_chip, 0)

        def f_wait(t, carry):
            f_arrived(nz - 1 - t).wait_recv()
            return carry

        def plane_table():
            lax.fori_loop(0, nz - 1 - z, f_wait, 0)

            @pl.when(z == nz - 1)
            def _():
                for source in range(half, nz - 1):
                    f_arrived(source).wait_recv()

            everything = jnp.concatenate(
                [
                    jnp.where((i > z) | (z == nz - 1 if half <= i < nz - 1 else False), fz_r[i, 0:1, :], 0.0)
                    for i in range(nz)
                ],
                axis=0,
            )
            th_s[0:nz, :] = everything

            def body(k, carry):
                rows = jnp.concatenate(split(th_s[...], 3), axis=1)
                for i in range(4):
                    fzx[4 * k + i] = dot(rows, indicator(4 * k + i, 3))
                return carry

            lax.fori_loop(0, QUARTERS // 4, body, 0)

        def within(g):
            bg = b_ref[:, lanes_of(g, N)]
            cg = c_ref[:, lanes_of(g, N)]
            cross = dot_nt(bg, cg)
            cols = pltpu.roll(cum_s[...], lax.rem(H - 16 * g, H), 1)
            low = lax.broadcasted_iota(jnp.int32, (T, T), 1) < D
            total = jnp.zeros((T, T), F32)
            for j in range(8):
                part = pl.ds(pl.multiple_of(1024 * g + 128 * j, 128), 128)
                gf = grad[:, part].astype(F32)
                xp = x_ref[:, part]
                both = jnp.concatenate(
                    [jnp.where(low, gf, 0.0).astype(BF16), jnp.where(low, 0.0, gf).astype(BF16)], axis=0
                )
                prod = dot_nt(both, xp)
                pieces = []
                for i in range(2):
                    j2 = 2 * j + i
                    spread = cols[:, j2 : j2 + 1] - cumt_s[pl.ds(16 * g + j2, 1), :]
                    total = total + jnp.exp(spread + bias_s[...]) * prod[T * i : T * i + T, :]
                    pieces.append((jnp.exp(biast_s[...] - spread) * cross).astype(BF16))
                out = dot(jnp.concatenate(pieces, axis=1), both)
                half = slice(128 * (j % 2), 128 * (j % 2) + 128)
                q = 4 * g + j // 2
                gxa[q, :, half] = out + thx[q, 8:9, half] * gf
            gca[g] = dot(total.astype(BF16), bg)
            gba[g] = dot(total.T.astype(BF16), cg)

        def sk_copy(off):
            return remote(sk_s, sk_r.at[d], ssend.at[off - 1], srecv.at[off - 1], plane_peer(off))

        def skz_copy(off):
            return remote(skz_s, skz_r.at[z], zsend.at[off - 1], zrecv.at[off - 1], z_peer(off))

        def sk_plane():
            row_q = lax.broadcasted_iota(jnp.int32, (QL, 128), 0)
            col_q = lax.broadcasted_iota(jnp.int32, (QL, 128), 1)
            pick = jnp.where(lax.shift_right_logical(row_q, 6) == (col_q & 3), 1.0, 0.0).astype(BF16)
            sums = jnp.reshape(skp[...], (QUARTERS, QL))
            heads = sum(dot(piece, pick) for piece in split(sums, 3))
            own_row = lax.broadcasted_iota(jnp.int32, (QUARTERS, 128), 0)
            own_col = lax.broadcasted_iota(jnp.int32, (QUARTERS, 128), 1)
            heads = jnp.where(lax.shift_right_logical(own_col, 2) == own_row, heads, 0.0)
            sk_s[...] = jnp.broadcast_to(jnp.sum(heads, axis=0, keepdims=True), (8, 128))
            sk_r[d] = sk_s[...]
            for off in range(1, 2 * NY):
                sk_copy(off).start()

        def sk_along():
            for off in range(1, 2 * NY):
                sk_copy(off).wait_recv()
            acc = sk_r[0]
            for i in range(1, 2 * NY):
                acc = acc + sk_r[i]
            skz_s[...] = acc
            skz_r[z] = acc
            for off in range(1, nz):
                skz_copy(off).start()

        def each(n, step):
            def body(k, carry):
                step(k)
                return carry

            lax.fori_loop(0, n, body, 0)

        def settle():
            @pl.when(px > 0)
            def _():
                each(CHUNKS, lambda k: grad_copy(k).wait_send())

            for off in range(1, 2 * NY):
                info_copy(off).wait_send()

            @pl.when((d == last_d) & (z < nz - 1))
            def _():
                for other in range(2 * NY):
                    info_next(other).wait_send()

            for w in range(2):

                def drain(k, w=w):
                    partner_copy(w, k).wait_send()
                    t_copy(w, k).wait_send()
                    u_copy(w, k).wait_send()
                    if w == 0:

                        @pl.when(z < nz - 1)
                        def _():
                            chain_copy(k).wait_send()
                    else:

                        def let_go(other, carry, k=k):
                            across(k, other).wait_send()
                            return carry

                        lax.fori_loop(start, z, let_go, 0)

                        @pl.when(to_top)
                        def _(k=k):
                            across(k, nz - 1).wait_send()

                each(count[w], drain)
            each(z, lambda other: f_copy(other).wait_send())

            @pl.when(to_top)
            def _():
                f_copy(nz - 1).wait_send()

        chain_at = 2 + lax.div(z * 5 + 3, nz - 1)
        back_at = jnp.where(z < half, 4, 3)

        def main(k, carry):
            def at(lag, n, step):
                @pl.when((k >= lag) & (k < lag + n))
                def _():
                    step(k - lag)

            def begin(k):
                @pl.when(px == nx - 1)
                def _():
                    for i in range(4):
                        part = lanes_of(4 * k + i, QL)
                        grad[:, part] = (grad[:, part].astype(F32) * wide_s[...]).astype(BF16)

                @pl.when(px < nx - 1)
                def _():
                    grad_copy(k).wait_recv()

                states(1, k, theirs)
                partner_copy(1, k).start()
                states(1, k, mine)

                @pl.when(k < CHUNKS - 1)
                def _():
                    enter_wide(k + 1, 0)

                chip_state(1, k)
                within(k)

            at(0, CHUNKS, begin)

            @pl.when(k == 1)
            def _():
                plane_table()

            def at_pairing_end(lag, n, step):
                @pl.when((k >= lag) & (k < lag + n - 1))
                def _():
                    step(k - lag)

                @pl.when(k == lag + n - 2)
                def _():
                    step(k - lag + 1)

            def two(step):
                def both(i):
                    step(2 * i)
                    step(2 * i + 1)

                return both

            at(1, count[1] - 1, lambda i: pair_step(1, i))
            at(2, count[1] - 2, plane_send)

            @pl.when(k == CHUNKS)
            def _():
                plane_send(CHUNKS - 1)
                sk_plane()

            at_pairing_end(back_at, count[1], plane_back)

            @pl.when(k == CHUNKS - 1)
            def _():
                pair_step(1, k)
                plane_send(k - 1)

            at_pairing_end(back_at + 1, count[1], lambda i: pair_out(1, i))
            at_pairing_end(back_at + 2, count[1], lambda i: hand_back(1, i))

            @pl.when(k == CHUNKS + 2)
            def _():
                sk_along()

            @pl.when(k == CHUNKS + 3)
            def _():
                settle()

            at_pairing_end(back_at + 3, count[1], finish_b)
            at(1, count[0] // 2, two(lambda i: pair_step(0, i)))

            @pl.when(z < nz - 1)
            def _():
                at(chain_at + 1, count[0], lambda i: pair_out(0, i))

            @pl.when(z == nz - 1)
            def _():
                at(chain_at + 1, count[0] // 2, two(lambda i: pair_out(0, i)))

            at(chain_at, count[0] // 2, two(chain))

            @pl.when(z < nz - 1)
            def _():
                at(chain_at + 2, count[0], lambda i: hand_back(0, i))

            @pl.when(z == nz - 1)
            def _():
                at(chain_at + 2, count[0] // 2, two(lambda i: hand_back(0, i)))

            at(chain_at + 3, count[0], finish_c)
            return carry

        lax.fori_loop(0, CHUNKS + 6, main, 0)

        for off in range(1, nz):
            skz_copy(off).wait_recv()
        acc = skz_r[0]
        for i in range(1, nz):
            acc = acc + skz_r[i]
        sk_out[...] = acc[0:1, :]

        for off in range(1, 2 * NY):
            sk_copy(off).wait_send()
        for off in range(1, nz):
            skz_copy(off).wait_send()

        for w in range(2):

            def drain(k, w=w):
                back_copy(w, k).wait_send()
                v_copy(w, k).wait_send()
                e_copy(w, k).wait_send()
                if w == 1:

                    @pl.when(z == half)
                    def _(k=k):
                        for other in nearer:
                            down(k, other).wait_send()

                    @pl.when(z == nz - 1)
                    def _(k=k):
                        for other in farther:
                            down(k, other).wait_send()

            each(count[w], drain)

    return kernel


def call(nx, nz):
    vm = pltpu.VMEM
    dma = pltpu.SemaphoreType.DMA
    scratch = [
        vm((T, H * D), BF16),
        vm((T, GROUPS * N), BF16),
        vm((T, GROUPS * N), BF16),
        vm((T, H), F32),
        dma((5,)),
        vm((T, H * D), BF16),
        vm((QUARTERS, T, QL), BF16),
        vm((QUARTERS, T, QL), BF16),
        vm((QUARTERS, T, QL), F32),
        vm((QUARTERS, T, QL), F32),
        vm((GROUPS, T, N), F32),
        vm((GROUPS, T, N), F32),
        vm((T, H), F32),
        vm((H, T), F32),
        vm((T, T), F32),
        vm((T, T), F32),
        vm((QUARTERS, T, QL), F32),
        vm((T, 2 * H), BF16),
        vm((T, 2 * H), BF16),
        vm((GROUPS, N, T), BF16),
        vm((GROUPS, N, T), BF16),
        vm((T, QL), F32),
        vm((8, H), F32),
        vm((nz, 8, H), F32),
        vm((QUARTERS, 16, QL), F32),
        vm((8, H), F32),
        vm((2 * NY + 1, 8, H), F32),
        vm((16, H), F32),
        vm((QUARTERS, 16, QL), F32),
        vm((2, 2, MINE, N, QL), BF16),
        vm((2, MINE, N, QL), BF16),
        vm((2, MINE, 2, 2 * ROWS, QL), BF16),
        vm((2, MINE, 2 * ROWS, QL), BF16),
        vm((2, MINE, 2, ROWS, QL), BF16),
        vm((2, MINE, ROWS, QL), BF16),
        vm((MINE, ROWS, QL), BF16),
        vm((MINE, ROWS, QL), BF16),
        vm((nz, MINE, ROWS, QL), BF16),
        vm((MINE, ROWS, QL), BF16),
        vm((MINE, ROWS, QL), BF16),
        vm((2, MINE, ROWS, QL), BF16),
        vm((2, MINE, 2, ROWS, QL), BF16),
        vm((2, MINE, 2 * ROWS, QL), BF16),
        vm((2, MINE, 2, 2 * ROWS, QL), BF16),
        vm((2, MINE, N, QL), BF16),
        vm((2, MINE, N, QL), BF16),
        vm((2, MINE, N, QL), BF16),
        vm((4, ROWS, QL), F32),
        vm((QUARTERS, 1, QL), F32),
        vm((8, 128), F32),
        vm((2 * NY, 8, 128), F32),
        vm((8, 128), F32),
        vm((nz, 8, 128), F32),
        dma((CHUNKS,)), dma((CHUNKS,)),
        dma((7 + 2 * NY,)), dma((8,)),
        dma((7,)), dma((7,)),
        dma((nz - 1,)), dma((nz - 1,)),
        dma((nz,)), dma((nz,)),
        dma((CHUNKS, nz)), dma((CHUNKS, nz)),
        dma((CHUNKS, nz)), dma((CHUNKS,)),
        dma((2, CHUNKS)), dma((2, CHUNKS)),
        dma((2, CHUNKS)), dma((2, CHUNKS)),
        dma((2, CHUNKS)), dma((2, CHUNKS)),
        dma((MINE // 4,)), dma((MINE // 4,)),
        dma((2, CHUNKS)), dma((2, CHUNKS)),
        dma((2, CHUNKS)), dma((2, CHUNKS)),
        dma((2, CHUNKS)), dma((2, CHUNKS)),
    ]
    return pl.pallas_call(
        make_kernel(nx, nz),
        out_shape=(
            vm((T, H * D), BF16),
            vm((T, GROUPS * N), BF16),
            vm((T, GROUPS * N), BF16),
            vm((1, H), F32),
        ),
        in_specs=[pl.BlockSpec(memory_space=pl.ANY)] * 5 + [pl.BlockSpec(memory_space=pltpu.VMEM)] * 4,
        out_specs=[pl.BlockSpec(memory_space=pltpu.VMEM)] * 4,
        scratch_shapes=scratch,
        compiler_params=pltpu.CompilerParams(vmem_limit_bytes=56 * 2**20, collective_id=0, has_side_effects=True),
        name="mixer_backward",
    )


def deliver(*results):
    def kernel(*refs):
        n = len(results)
        sem = refs[2 * n]
        copies = [pltpu.make_async_copy(refs[i], refs[n + i], sem.at[i]) for i in range(n)]
        for copy in copies:
            copy.start()
        for copy in copies:
            copy.wait()

    return pl.pallas_call(
        kernel,
        out_shape=tuple(jax.ShapeDtypeStruct(v.shape, v.dtype) for v in results),
        in_specs=[pl.BlockSpec(memory_space=pltpu.VMEM)] * len(results),
        out_specs=[pl.BlockSpec(memory_space=pl.ANY)] * len(results),
        scratch_shapes=[pltpu.SemaphoreType.DMA((len(results),))],
        compiler_params=pltpu.CompilerParams(vmem_limit_bytes=2**20),
        name="deliver",
    )(*results)


def on_device(previous, saved_head_inputs, input_b, input_c, steps, decay_rate, skip_gain, segment_ids, advantage_mask):
    kernel = call(lax.axis_size("pipe"), lax.axis_size("seq_0"))
    gx, gb, gc, sk = kernel(
        previous[0],
        saved_head_inputs[0],
        input_b[0],
        input_c[0],
        steps[0],
        decay_rate,
        skip_gain,
        segment_ids,
        advantage_mask[None],
    )
    gx, gb, gc, sk = deliver(gx, gb, gc, sk)
    return gx[None], gb[None], gc[None], sk


def solution(mesh):
    finer = Mesh(
        mesh.devices.reshape(mesh.shape["pipe"], mesh.shape["seq"] // (2 * NY), NY, 2),
        ("pipe", "seq_0", "seq_1", "seq_2"),
    )
    return jax.shard_map(
        on_device,
        mesh=finer,
        in_specs=(
            P("pipe", SEQ, None),
            P("pipe", SEQ, None),
            P("pipe", SEQ, None),
            P("pipe", SEQ, None),
            P("pipe", SEQ, None),
            P("pipe", None),
            P("pipe", None),
            P("pipe", SEQ),
            P(SEQ),
        ),
        out_specs=(
            P("pipe", SEQ, None),
            P("pipe", SEQ, None),
            P("pipe", SEQ, None),
            P("pipe", None),
        ),
        check_vma=False,
    )
```
